512 devices in a mesh: seg: 128 (over y, z, core), sp: 4 (over x).
Axes of the slice: x: 4, y: 4, z: 16, core: 2. Of those that a mesh axis runs over, the one named last changes fastest.
Arguments:
- coeffs: float32 [8, 2048, 680], P('sp', 'seg'), may hold values from -0.6 to 0.6
- points: float32 [3, 2048, 768], P(None, 'seg'), may hold values from -1 to 1
- owner_leaf: int32 [2048, 6], P('seg'), may hold values from 0 to 2047, as said below
- reaction: float32 [8, 8], replicated, may hold values from -2 to 2
- fit_matrix: float32 [768, 680], replicated, may hold values from -0.21875 to 0.21875
- new_seg: int32 [2048], replicated, may hold values from 0 to 127, as said below
- near_src: int32 [2048, 16], replicated, may hold values from -1 to 2047, as said below
- near_op: int32 [2048, 16], replicated, may hold values from 0 to 1
- near_mat: bfloat16 [2, 680, 680], replicated, may hold values from -0.0546875 to 0.0546875
- up_mat: bfloat16 [680, 152], replicated, may hold values from -0.21875 to 0.21875
- far_src: int32 [2048, 8], replicated, may hold values from -1 to 2047, as said below
- trans_mat: bfloat16 [8, 152, 152], replicated, may hold values from -0.15625 to 0.15625
- down_mat: bfloat16 [152, 680], replicated, may hold values from -0.5 to 0.5
Outputs:
- updated: float32 [8, 3072, 680], P('sp', 'seg')
The draws below stay inside these ranges and needn't reach their ends.
Inputs may be any that keep to these rules, and one draw needn't show every extreme that they name: `owner_leaf`: of the 96 blocks of one segment's leaves, at most 2 have their owner among the 16 leaves of any one segment. `new_seg`: never falls along the leaves; leaf t goes to segment t // 16, or to the one before only if t % 16 < 4, or to the one after only if t % 16 >= 12. `near_src`: -1 marks an unused entry; any other entry differs from its row's leaf index by at most 4. `far_src`: -1 marks an absent interaction.
All inputs are finite; a program needn't handle non-finite values.
Results may differ from the reference program's by a relative error of at most 0.0035.
Values may be sent and summed in bfloat16 or wider, within the bound.
No kernel may reach another device: no remote copies, remote signals or barrier semaphores. Data moves between devices by JAX's collectives and lax.ppermute only.
A program may use at most 64 MiB of HBM per device.

```python
import jax
import jax.numpy as jnp
import numpy as np
from jax import lax

SPECIES = 8
ORDER = 14
C = 680
Q = 152
NODES = 768
PB = 128
BLOCKS = 6
LEAF_DEV = 16
LEAVES = 2048
CAP = 2
MOVE = 4
REACH = 4
MAXL = 24
SLOTS = 3072
NEAR = 16
NEAR_OPS = 2
NOPS = 8
N_SEG = 128


def draw_owner_leaf(key, part):
    segment_total = LEAVES // LEAF_DEV
    per_device = LEAF_DEV * BLOCKS
    hot_segment = jax.random.randint(jax.random.fold_in(key, 1), (), 0, segment_total)

    def one_device(device_key):
        spread = jax.random.permutation(jax.random.fold_in(device_key, 2), (segment_total - 1) * CAP)[:per_device - CAP]
        offsets = jnp.concatenate([jnp.zeros((CAP,), jnp.int32), 1 + spread.astype(jnp.int32) // CAP])
        shuffled = offsets[jax.random.permutation(jax.random.fold_in(device_key, 3), per_device)]
        local_leaf = jax.random.randint(jax.random.fold_in(device_key, 4), (per_device,), 0, LEAF_DEV)
        return (hot_segment + shuffled) % segment_total * LEAF_DEV + local_leaf
    device_keys = jax.vmap(lambda device: jax.random.fold_in(key, device + 10))(jnp.arange(segment_total))
    return jax.vmap(one_device)(device_keys).reshape(LEAVES, BLOCKS).astype(jnp.int32)


def draw_new_seg(key, part):
    segment_total = LEAVES // LEAF_DEV
    shifts = jax.random.randint(jax.random.fold_in(key, 1), (segment_total + 1,), -MOVE, MOVE + 1)
    chosen = jax.random.randint(jax.random.fold_in(key, 2), (), 1, segment_total)
    border = jnp.arange(segment_total + 1, dtype=jnp.int32)
    shifts = jnp.where(border == chosen, MOVE, shifts)
    bounds = border * LEAF_DEV + shifts
    bounds = jnp.where(border == 0, 0, jnp.where(border == segment_total, LEAVES, bounds))
    leaf_index = jnp.arange(LEAVES, dtype=jnp.int32)
    home = leaf_index // LEAF_DEV
    later = (leaf_index >= bounds[home]).astype(jnp.int32) + (leaf_index >= bounds[home + 1]).astype(jnp.int32)
    return (home - 1 + later).astype(jnp.int32)


def draw_near_src(key, part):
    leaf_index = jnp.arange(LEAVES, dtype=jnp.int32)[:, None]
    column = jnp.arange(NEAR, dtype=jnp.int32)[None, :]
    offsets = jax.random.randint(jax.random.fold_in(key, 1), (LEAVES, NEAR), -REACH, REACH + 1)
    kept_entry = jax.random.randint(jax.random.fold_in(key, 2), (LEAVES, NEAR), 0, 8) > 0
    special = jax.random.randint(jax.random.fold_in(key, 3), (), 0, LEAVES - REACH)
    forced = (leaf_index == special) & (column == 0)
    offsets = jnp.where(forced, REACH, offsets)
    kept_entry = kept_entry | forced
    source = leaf_index + offsets
    usable = kept_entry & (source >= 0) & (source < LEAVES)
    return jnp.where(usable, source, -1).astype(jnp.int32)


def draw_far_src(key, part):
    source = jax.random.randint(jax.random.fold_in(key, 5), (LEAVES, NOPS), 0, LEAVES)
    kept_entry = jax.random.randint(jax.random.fold_in(key, 6), (LEAVES, NOPS), 0, 8) > 0
    return jnp.where(kept_entry, source, -1).astype(jnp.int32)


def set_ends(drawn, own_key, smallest, largest):
    spot = [jax.random.randint(jax.random.fold_in(own_key, axis), (), 0, length) for axis, length in enumerate(drawn.shape)]
    main_axis = drawn.shape.index(max(drawn.shape))
    next_to = spot[:main_axis] + [(spot[main_axis] + 1) % drawn.shape[main_axis]] + spot[main_axis + 1:]
    return drawn.at[tuple(spot)].set(smallest).at[tuple(next_to)].set(largest)


def block_scale(rng, extent, cuts, low, high):
    def one(axis_at, parts):
        heights = jax.random.uniform(jax.random.fold_in(jax.random.fold_in(rng, 6), axis_at), (parts,), jnp.float32, low / len(cuts), high / len(cuts))
        return jnp.repeat(jnp.exp(heights), extent[axis_at] // parts).reshape((-1,) + (1,) * (len(extent) - axis_at - 1))

    loudness = one(*cuts[0])
    for cut in cuts[1:]:
        loudness = loudness * one(*cut)
    return loudness


def noise(rng, dims, scale, reach, split=(), kind=jnp.bfloat16):
    drawn = jax.random.normal(rng, dims, jnp.float32) * scale
    if len(split) > 0:
        drawn = block_scale(rng, dims, split, -0.22, 0.18) * drawn
    return jnp.clip(drawn, min=-reach, max=reach).astype(kind)


def setup_inputs(seed: int = 0) -> dict:
    arg_keys = jax.random.split(jax.random.key(seed), 14)
    return {
        "coeffs": noise(arg_keys[0], (SPECIES, LEAVES, C), 0.1, 0.6, ((0, 4), (1, 128)), jnp.float32),
        "points": jnp.clip(jax.random.uniform(arg_keys[1], (3, LEAVES, NODES), jnp.float32, -1.0, 1.0) * block_scale(arg_keys[1], (3, LEAVES, NODES), ((1, 128),), -0.4, 0.0), -1.0, 1.0),
        "owner_leaf": draw_owner_leaf(jax.random.fold_in(arg_keys[13], 71), 0),
        "reaction": noise(arg_keys[3], (SPECIES, SPECIES), SPECIES ** -0.5, 2.0, (), jnp.float32),
        "fit_matrix": noise(arg_keys[4], (NODES, C), NODES ** -0.5, 0.21875, (), jnp.float32),
        "new_seg": draw_new_seg(jax.random.fold_in(arg_keys[13], 71), 0),
        "near_src": draw_near_src(jax.random.fold_in(arg_keys[13], 71), 0),
        "near_op": set_ends(jax.random.randint(arg_keys[7], (LEAVES, NEAR), 0, NEAR_OPS), jax.random.fold_in(arg_keys[7], 1), 0, NEAR_OPS - 1).astype(jnp.int32),
        "near_mat": noise(arg_keys[8], (NEAR_OPS, C, C), (C * NEAR) ** -0.5, 0.0546875),
        "up_mat": noise(arg_keys[9], (C, Q), C ** -0.5, 0.21875),
        "far_src": draw_far_src(jax.random.fold_in(arg_keys[13], 71), 0),
        "trans_mat": noise(arg_keys[11], (NOPS, Q, Q), (Q * NOPS) ** -0.5, 0.15625),
        "down_mat": noise(arg_keys[12], (Q, C), Q ** -0.5, 0.5),
    }


precise = lax.Precision.HIGHEST


def basis_tables(order):
    pair_list = [(deg_x, deg_y) for deg_x in range(order + 1) for deg_y in range(order + 1 - deg_x)]
    total_width = (order + 1) * (order + 2) * (order + 3) // 6
    lookup = np.full((len(pair_list), order + 1), total_width, np.int32)
    x_select = np.zeros((len(pair_list), order + 1), np.float32)
    y_select = np.zeros((len(pair_list), order + 1), np.float32)
    counter = 0
    for row_number, (deg_x, deg_y) in enumerate(pair_list):
        x_select[row_number, deg_x] = 1.0
        y_select[row_number, deg_y] = 1.0
        for deg_z in range(order + 1 - deg_x - deg_y):
            lookup[row_number, deg_z] = counter
            counter += 1
    return lookup, x_select, y_select


def chebyshev(position_values, order):
    polynomials = [jnp.ones_like(position_values), position_values]
    for degree in range(2, order + 1):
        polynomials.append(2.0 * position_values * polynomials[-1] - polynomials[-2])
    return jnp.stack(polynomials[: order + 1], axis=-2)


def evaluate(coefficient, coords):
    lookup, x_select, y_select = basis_tables(ORDER)
    padded = jnp.concatenate([coefficient, jnp.zeros(coefficient.shape[:-1] + (1,), coefficient.dtype)], axis=-1)
    dense_coef = jnp.take(padded, jnp.asarray(lookup), axis=-1)
    along_x = chebyshev(coords[0], ORDER)
    along_y = chebyshev(coords[1], ORDER)
    along_z = chebyshev(coords[2], ORDER)
    inner_sum = jnp.einsum('sqk,kp->sqp', dense_coef, along_z, precision=precise)
    y_rows = jnp.einsum('qk,kp->qp', jnp.asarray(y_select, coefficient.dtype), along_y, precision=precise)
    folded = jnp.einsum('sqp,qk->skp', inner_sum * y_rows[None], jnp.asarray(x_select, coefficient.dtype), precision=precise)
    return jnp.sum(folded * along_x[None], axis=1)


def reference(coeffs, points, owner_leaf, reaction, fit_matrix, new_seg, near_src, near_op, near_mat, up_mat, far_src, trans_mat, down_mat):
    coords = points.reshape(3, LEAVES * BLOCKS, PB).transpose(1, 0, 2)
    flat_owner = owner_leaf.reshape(-1).astype(jnp.int32)

    def per_block(block_args):
        coefficient = jnp.take(coeffs, block_args[0], axis=1)
        return evaluate(coefficient, block_args[1])

    values = lax.map(per_block, (flat_owner, coords), batch_size=64)
    values = values.reshape(LEAVES, BLOCKS, SPECIES, PB).transpose(2, 0, 1, 3).reshape(SPECIES, LEAVES, NODES)
    mixing = jnp.einsum('sr,rln->sln', reaction, values, precision=precise)
    reacted = values + jnp.tanh(mixing)
    refitted = jnp.einsum('sln,nc->slc', reacted, fit_matrix, precision=precise)
    ghosts = lax.optimization_barrier(refitted.astype(jnp.bfloat16))
    ghost_wide = ghosts.astype(jnp.float32)
    equivalent = jnp.einsum('slc,cq->slq', ghost_wide, up_mat.astype(jnp.float32), precision=precise).astype(jnp.bfloat16)
    equiv_wide = lax.optimization_barrier(equivalent).astype(jnp.float32)
    near_wide = near_mat.astype(jnp.float32)
    trans_wide = trans_mat.astype(jnp.float32)
    down_wide = down_mat.astype(jnp.float32)

    def per_segment(segment):
        target = segment * LEAF_DEV - MOVE + jnp.arange(MAXL, dtype=jnp.int32)
        inside = (target >= 0) & (target < LEAVES)
        clipped = jnp.clip(target, 0, LEAVES - 1).astype(jnp.int32)
        live_slot = inside & (new_seg[clipped] == segment)
        own_term = jnp.take(ghost_wide, clipped, axis=1)
        near_from = near_src[clipped]
        near_kind = near_op[clipped]
        near_ok = live_slot[:, None] & (near_from >= 0)
        picked = jnp.take(ghost_wide, jnp.clip(near_from, 0, LEAVES - 1).reshape(-1).astype(jnp.int32), axis=1)
        picked = picked.reshape(SPECIES, MAXL, NEAR, C)
        near_term = jnp.zeros((SPECIES, MAXL, C), jnp.float32)
        for operator in range(NEAR_OPS):
            weight_mask = (near_ok & (near_kind == operator)).astype(picked.dtype)
            grouped = jnp.sum(picked * weight_mask[None, :, :, None], axis=2)
            near_term = near_term + jnp.einsum('sjc,cd->sjd', grouped, near_wide[operator], precision=precise)
        far_from = far_src[clipped]
        far_ok = (live_slot[:, None] & (far_from >= 0)).astype(equiv_wide.dtype)
        far_rows = jnp.take(equiv_wide, jnp.clip(far_from, 0, LEAVES - 1).reshape(-1).astype(jnp.int32), axis=1)
        far_rows = far_rows.reshape(SPECIES, MAXL, NOPS, Q) * far_ok[None, :, :, None]
        local_expansion = jnp.einsum('sjoq,oqr->sjr', far_rows, trans_wide, precision=precise).astype(jnp.bfloat16)
        local_expansion = lax.optimization_barrier(local_expansion).astype(jnp.float32)
        far_term = jnp.einsum('sjq,qc->sjc', local_expansion, down_wide, precision=precise)
        total = own_term + near_term + far_term
        return jnp.where(live_slot[None, :, None], total, jnp.zeros_like(total))

    updated = lax.map(per_segment, jnp.arange(N_SEG, dtype=jnp.int32))
    return updated.transpose(1, 0, 2, 3).reshape(SPECIES, SLOTS, C)
```

```python
import functools

import jax
import jax.numpy as jnp
import numpy as np
from jax import lax
from jax.experimental import pallas as pl
from jax.experimental.pallas import tpu as pltpu
from jax.sharding import Mesh
from jax.sharding import PartitionSpec as P

ORDER = 14
DEG = ORDER + 1
BLOCKS = 6
PB = 128
MOVE = 4
REACH = 4
MARGIN = MOVE + REACH
CAP = 2
PAIR_ROWS = 128
LANES = 384
SEG = ("seg_0", "seg_1", "seg_2")
F32 = jnp.float32
BF16 = jnp.bfloat16


def degree_pairs():
    return [(i, d - i) for d in range(DEG) for i in range(d + 1)]


def coefficient_table():
    number = {}
    for i in range(DEG):
        for j in range(DEG - i):
            for k in range(DEG - i - j):
                number[i, j, k] = len(number)
    table = np.full((DEG, PAIR_ROWS), -1, np.int32)
    for k in range(DEG):
        for q, (i, j) in enumerate(degree_pairs()):
            if i + j + k <= ORDER:
                table[k, q] = number[i, j, k]
    return table.reshape(1, DEG * PAIR_ROWS)


def high_low(value):
    high = value.astype(BF16)
    return high, (value - high.astype(F32)).astype(BF16)


def polynomials(x):
    terms = [jnp.ones_like(x), x]
    for _ in range(2, DEG):
        terms.append(2.0 * x * terms[-1] - terms[-2])
    return terms


def route_kernel(part_ref, owner_ref, points_ref, request_ref, place_ref, count_ref, line_ref):
    part = part_ref[0]
    leaves, blocks = owner_ref.shape
    coordinate = jnp.minimum(part, 2)
    request_ref[...] = jnp.zeros_like(request_ref)
    for m in range(blocks):
        line_ref[m * leaves : (m + 1) * leaves] = points_ref[coordinate, :, m * PB : (m + 1) * PB]

    @pl.loop(0, count_ref.shape[0])
    def _(d):
        count_ref[d] = 0

    @pl.loop(0, leaves)
    def _(leaf):
        for m in range(blocks):
            owner = owner_ref[leaf, m]
            target = lax.shift_right_logical(owner, 4)
            used = count_ref[target]
            count_ref[target] = used + 1
            row = target * CAP + used
            place_ref[leaf * blocks + m] = row
            line = line_ref[pl.ds(m * leaves + leaf, 1), :]
            index = jnp.full((1, PB), (owner & 15).astype(F32), F32)
            request_ref[pl.ds(row, 1), :] = jnp.where(part == 3, index, line)


def evaluate_kernel(index_ref, request_ref, coeffs_ref, table_ref, out_ref, split_ref, left_ref, pair_ref, z_ref):
    species, leaves, width = coeffs_ref.shape
    per_leaf = 4 * 16
    split_ref[...] = jnp.zeros_like(split_ref)
    parts = []
    for s in range(species):
        parts.append(coeffs_ref[s])
    both = jnp.concatenate(parts, axis=0)
    rest = both - both.astype(BF16).astype(F32)
    stacked = jnp.concatenate([both, rest], axis=0).astype(BF16)
    for k in range(DEG):
        wanted = table_ref[:, k * PAIR_ROWS : (k + 1) * PAIR_ROWS]
        rows = lax.broadcasted_iota(jnp.int32, (width, PAIR_ROWS), 0)
        pick = jnp.where(rows == wanted, 1.0, 0.0).astype(BF16)
        moved = jnp.dot(stacked, pick, preferred_element_type=F32)
        for h in range(2 * species):
            split_ref[pl.ds(h * 16 + k, leaves, stride=per_leaf), :] = moved[h * leaves : (h + 1) * leaves]

    @pl.loop(0, leaves)
    def _(leaf):
        block = split_ref[pl.ds(leaf * per_leaf, per_leaf), :]
        half = per_leaf // 2
        upper = jnp.concatenate([block[:half], jnp.zeros_like(block[:half])], axis=0)
        left_ref[leaf] = jnp.concatenate([block, upper], axis=1).astype(BF16)

    for i in range(8):
        pair_ref[pl.ds(i * PAIR_ROWS + 120, 8), :] = jnp.zeros((8, PB), F32)
        z_ref[pl.ds(i * 16 + 8, 8), :] = jnp.zeros((8, PB), F32)

    @pl.loop(0, request_ref.shape[1] // 8)
    def _(group):
        at = pl.ds(pl.multiple_of(group * 8, 8), 8)
        along_x = polynomials(request_ref[0, at, :])
        along_y = polynomials(request_ref[1, at, :])
        along_z = polynomials(request_ref[2, at, :])
        for q, (i, j) in enumerate(degree_pairs()):
            product = along_x[i] if j == 0 else along_y[j] if i == 0 else along_x[i] * along_y[j]
            pair_ref[pl.ds(q, 8, stride=PAIR_ROWS), :] = product
        for k in range(DEG):
            z_ref[pl.ds(k, 8, stride=16), :] = along_z[k]
        for i in range(8):
            high, low = high_low(pair_ref[pl.ds(i * PAIR_ROWS, PAIR_ROWS), :])
            right = jnp.concatenate([high, low], axis=0)
            leaf = index_ref[group * 8 + i]
            sums = jnp.dot(left_ref[leaf], right, preferred_element_type=F32)
            sums = sums[:32] + sums[32:]
            weight = z_ref[pl.ds(i * 16, 16), :]
            for s in range(species):
                line = jnp.sum(sums[s * 16 : (s + 1) * 16] * weight, axis=0, keepdims=True)
                out_ref[pl.ds(group * 16 + i * 2 + s, 1), :] = line


def collect_kernel(place_ref, rows_ref, out_ref, line_ref):
    species, leaves, nodes = out_ref.shape

    @pl.loop(0, leaves)
    def _(leaf):
        for m in range(BLOCKS):
            row = place_ref[leaf * BLOCKS + m]
            for s in range(species):
                at = (s * BLOCKS + m) * leaves + leaf
                line_ref[pl.ds(at, 1), :] = rows_ref[pl.ds(row * species + s, 1), :]

    for s in range(species):
        for m in range(BLOCKS):
            at = (s * BLOCKS + m) * leaves
            out_ref[s, :, m * PB : (m + 1) * PB] = line_ref[at : at + leaves]


def fit_kernel(part_ref, reaction_ref, values_ref, fit_ref, up_ref, ghosts_ref, equivalent_ref):
    part = part_ref[0]
    all_species = values_ref.shape[0]
    species, leaves, width = ghosts_ref.shape
    reacted = []
    for s in range(species):
        row = part * species + s
        mixing = reaction_ref[row, 0] * values_ref[0]
        for r in range(1, all_species):
            mixing = mixing + reaction_ref[row, r] * values_ref[r]
        reacted.append(values_ref[row] + jnp.tanh(mixing))
    reacted = jnp.concatenate(reacted, axis=0)
    rows = species * leaves
    high = reacted.astype(BF16)
    stacked = jnp.concatenate([reacted, reacted - high.astype(F32)], axis=0).astype(BF16)
    fit_high, fit_low = high_low(fit_ref[...])
    first = jnp.dot(stacked, fit_high, preferred_element_type=F32)
    second = jnp.dot(high, fit_low, preferred_element_type=F32)
    ghosts = (first[:rows] + first[rows:] + second).astype(BF16)
    equivalent = jnp.dot(ghosts, up_ref[...], preferred_element_type=F32).astype(BF16)
    points = up_ref.shape[1]
    equivalent_ref[...] = jnp.zeros_like(equivalent_ref)
    for s in range(species):
        ghosts_ref[s] = ghosts[s * leaves : (s + 1) * leaves]
        equivalent_ref[:, s * points : (s + 1) * points] = equivalent[s * leaves : (s + 1) * leaves]


def update_kernel(
    where_ref, before_ref, ghosts_ref, after_ref, near_src_ref, near_op_ref, far_src_ref, live_ref,
    near_mat_ref, mine_ref, other_ref, trans_ref, down_ref, out_ref, wide_ref,
):
    segment = where_ref[0]
    core = where_ref[1]
    species, slots, width = out_ref.shape
    leaves = ghosts_ref.shape[1]
    live = live_ref[...] > 0
    span = leaves + 2 * MARGIN
    source = near_src_ref[...]
    offset = jnp.where(live & (source >= 0), source - (segment * leaves - MARGIN), -1)
    kind = near_op_ref[...]
    columns = lax.broadcasted_iota(jnp.int32, (slots, span), 1)
    weights = []
    for o in range(near_mat_ref.shape[0]):
        chosen = jnp.where(kind == o, offset, -1)
        weight = jnp.zeros((slots, span), F32)
        for q in range(source.shape[1]):
            weight = weight + jnp.where(chosen[:, q : q + 1] == columns, 1.0, 0.0)
        weights.append(weight)
    own = []
    around = []
    for s in range(species):
        wide_ref[s, 0:MARGIN, :] = before_ref[s].astype(F32)
        wide_ref[s, MARGIN : MARGIN + leaves, :] = ghosts_ref[s].astype(F32)
        wide_ref[s, MARGIN + leaves : span, :] = after_ref[s].astype(F32)
        own.append(wide_ref[s, MOVE : MOVE + slots, :])
        around.append(wide_ref[s].astype(BF16))
    total = jnp.concatenate(own, axis=0)
    rows = species * slots
    for o in range(near_mat_ref.shape[0]):
        weight = weights[o].astype(BF16)
        grouped = jnp.concatenate(
            [jnp.dot(weight, around[s], preferred_element_type=F32) for s in range(species)], axis=0
        )
        rest = grouped - grouped.astype(BF16).astype(F32)
        stacked = jnp.concatenate([grouped, rest], axis=0).astype(BF16)
        term = jnp.dot(stacked, near_mat_ref[o], preferred_element_type=F32)
        total = total + term[:rows] + term[rows:]

    far = far_src_ref[...]
    far_segment = lax.shift_right_logical(far, 4)
    far_row = lax.shift_right_logical(far_segment, 1) * leaves + (far & 15)
    far_ok = live & (far >= 0)
    here = (far_segment & 1) == core
    mine_row = jnp.where(far_ok & here, far_row, -1)
    other_row = jnp.where(far_ok & jnp.logical_not(here), far_row, -1)
    operators = far.shape[1]
    held = mine_ref.shape[0]
    taken = None
    for row, table in ((mine_row, mine_ref), (other_row, other_ref)):
        column = jnp.concatenate([row[:, o : o + 1] for o in range(operators)], axis=0)
        ids = lax.broadcasted_iota(jnp.int32, (operators * slots, held), 1)
        pick = jnp.where(column == ids, 1.0, 0.0).astype(BF16)
        part = jnp.dot(pick, table[...], preferred_element_type=F32)
        taken = part if taken is None else taken + part
    points = trans_ref.shape[1]
    local = None
    for o in range(operators):
        lines = taken[o * slots : (o + 1) * slots]
        both = jnp.concatenate([lines[:, s * points : (s + 1) * points] for s in range(species)], axis=0)
        term = jnp.dot(both.astype(BF16), trans_ref[o], preferred_element_type=F32)
        local = term if local is None else local + term
    total = total + jnp.dot(local.astype(BF16), down_ref[...], preferred_element_type=F32)
    for s in range(species):
        out_ref[s] = jnp.where(live, total[s * slots : (s + 1) * slots], 0.0)


def spaces(text):
    names = {"s": pltpu.SMEM, "v": pltpu.VMEM}
    return [pl.BlockSpec(memory_space=names[c]) for c in text]


def within(mebibytes):
    return pltpu.CompilerParams(vmem_limit_bytes=mebibytes * 1024 * 1024)


def shards(
    coeffs, points, owner_leaf, reaction, fit_matrix, new_seg, near_src, near_op, near_mat, up_mat,
    far_src, trans_mat, down_mat,
):
    species, leaves, width = coeffs.shape
    segments = lax.axis_size(SEG)
    segment = lax.axis_index(SEG)
    part = lax.axis_index("sp")
    part_id = jnp.full((1,), part, jnp.int32)
    slots = segments * CAP
    shape = jax.ShapeDtypeStruct

    request, place = pl.pallas_call(
        route_kernel,
        out_shape=(shape((slots, PB), F32), shape((leaves * BLOCKS,), jnp.int32)),
        in_specs=spaces("ssv"),
        out_specs=tuple(spaces("vs")),
        scratch_shapes=[pltpu.SMEM((segments,), jnp.int32), pltpu.VMEM((leaves * BLOCKS, PB), F32)],
        compiler_params=within(4),
    )(part_id, owner_leaf, points)
    request = lax.all_to_all(request.reshape(segments, CAP, PB), SEG, 0, 0, tiled=True)
    request = lax.all_gather(request.reshape(slots, PB), "sp", axis=0)
    index = jnp.clip(request[3, :, 0].astype(jnp.int32), 0, leaves - 1)
    answers = pl.pallas_call(
        evaluate_kernel,
        out_shape=shape((slots * species, PB), F32),
        in_specs=spaces("svvv"),
        out_specs=spaces("v")[0],
        scratch_shapes=[
            pltpu.VMEM((leaves * 64, PB), F32),
            pltpu.VMEM((leaves, 64, 2 * PB), BF16),
            pltpu.VMEM((8 * PAIR_ROWS, PB), F32),
            pltpu.VMEM((8 * 16, PB), F32),
        ],
        compiler_params=within(16),
    )(index, request, coeffs, jnp.asarray(coefficient_table()))
    answers = lax.all_to_all(answers.reshape(segments, CAP * species, PB), SEG, 0, 0, tiled=True)
    values = pl.pallas_call(
        collect_kernel,
        out_shape=shape((species, leaves, BLOCKS * PB), F32),
        in_specs=spaces("sv"),
        out_specs=spaces("v")[0],
        scratch_shapes=[pltpu.VMEM((species * leaves * BLOCKS, PB), F32)],
        compiler_params=within(4),
    )(place, answers.reshape(slots * species, PB))
    gathered = lax.all_gather(values, "sp", axis=0, tiled=True)
    ghosts, equivalent = pl.pallas_call(
        fit_kernel,
        out_shape=(shape((species, leaves, width), BF16), shape((leaves, LANES), BF16)),
        in_specs=spaces("ssvvv"),
        out_specs=tuple(spaces("vv")),
        compiler_params=within(24),
    )(part_id, reaction, gathered, fit_matrix, up_mat)

    up = [(i, i + 1) for i in range(segments - 1)]
    down = [(j, i) for i, j in up]
    before = lax.ppermute(ghosts[:, leaves - MARGIN :], SEG, up)
    after = lax.ppermute(ghosts[:, :MARGIN], SEG, down)

    z_size = lax.axis_size("seg_1")
    spread = jnp.broadcast_to(equivalent[None], (z_size, leaves, LANES))
    along_z = lax.all_to_all(spread, "seg_1", 0, 0, tiled=True)
    mine = lax.all_gather(along_z.reshape(z_size * leaves, LANES), "seg_0", axis=0, tiled=True)
    other = lax.ppermute(mine, "seg_2", [(0, 1), (1, 0)])

    slot_total = leaves + 2 * MOVE
    leaf_total = new_seg.shape[0]
    target = segment * leaves - MOVE + jnp.arange(slot_total, dtype=jnp.int32)
    inside = (target >= 0) & (target < leaf_total)
    clipped = jnp.clip(target, 0, leaf_total - 1)
    live = (inside & (new_seg[clipped] == segment)).astype(jnp.int32)[:, None]
    where = jnp.stack([segment, lax.axis_index("seg_2")]).astype(jnp.int32)
    return pl.pallas_call(
        update_kernel,
        out_shape=shape((species, slot_total, width), F32),
        in_specs=spaces("svvvvvvvvvvvv"),
        out_specs=spaces("v")[0],
        scratch_shapes=[pltpu.VMEM((species, leaves + 2 * MARGIN, width), F32)],
        compiler_params=within(24),
    )(
        where, before, ghosts, after, near_src[clipped], near_op[clipped], far_src[clipped], live,
        near_mat, mine, other, trans_mat, down_mat,
    )


def solution(mesh):
    torus = Mesh(
        mesh.devices.reshape(4, 16, 2, mesh.shape["sp"]), ("seg_0", "seg_1", "seg_2", "sp")
    )
    whole = P()
    return jax.shard_map(
        shards,
        mesh=torus,
        in_specs=(P("sp", SEG, None), P(None, SEG, None), P(SEG, None)) + (whole,) * 10,
        out_specs=P("sp", SEG, None),
        check_vma=False,
    )
```

```python
import functools

import jax
import jax.numpy as jnp
import numpy as np
from jax import lax
from jax.experimental import pallas as pl
from jax.experimental.pallas import tpu as pltpu
from jax.sharding import Mesh
from jax.sharding import PartitionSpec as P

ORDER = 14
DEG = ORDER + 1
BLOCKS = 6
PB = 128
MOVE = 4
REACH = 4
MARGIN = MOVE + REACH
CAP = 2
PAIR_ROWS = 128
LANES = 384
SEG = ("seg_0", "seg_1", "seg_2")
F32 = jnp.float32
BF16 = jnp.bfloat16


def degree_pairs():
    pairs = []
    for i in range(8):
        for r in range(16):
            pairs.append((i, r) if r < DEG - i else (DEG - i, r - (DEG - i)))
    return pairs


def coefficient_table():
    number = {}
    for i in range(DEG):
        for j in range(DEG - i):
            for k in range(DEG - i - j):
                number[i, j, k] = len(number)
    table = np.full((DEG, PAIR_ROWS), -1, np.int32)
    for k in range(DEG):
        for q, (i, j) in enumerate(degree_pairs()):
            if i + j + k <= ORDER:
                table[k, q] = number[i, j, k]
    return table.reshape(1, DEG * PAIR_ROWS)


def high_low(value):
    high = value.astype(BF16)
    return high, (value - high.astype(F32)).astype(BF16)


def polynomials(x):
    terms = [jnp.ones_like(x), x]
    for _ in range(2, DEG):
        terms.append(2.0 * x * terms[-1] - terms[-2])
    return terms


def route_kernel(part_ref, owner_ref, points_ref, request_ref, place_ref, count_ref, line_ref):
    part = part_ref[0]
    leaves, blocks = owner_ref.shape
    coordinate = jnp.minimum(part, 2)
    request_ref[...] = jnp.zeros_like(request_ref)
    for m in range(blocks):
        line_ref[m * leaves : (m + 1) * leaves] = points_ref[coordinate, :, m * PB : (m + 1) * PB]

    @pl.loop(0, count_ref.shape[0])
    def _(d):
        count_ref[d] = 0

    @pl.loop(0, leaves)
    def _(leaf):
        for m in range(blocks):
            owner = owner_ref[leaf, m]
            target = lax.shift_right_logical(owner, 4)
            used = count_ref[target]
            count_ref[target] = used + 1
            row = target * CAP + used
            place_ref[leaf * blocks + m] = row
            line = line_ref[pl.ds(m * leaves + leaf, 1), :]
            index = jnp.full((1, PB), (owner & 15).astype(F32), F32)
            request_ref[pl.ds(row, 1), :] = jnp.where(part == 3, index, line)


def evaluate_kernel(index_ref, request_ref, coeffs_ref, table_ref, out_ref, split_ref, left_ref, x_ref, y_ref, z_ref):
    species, leaves, width = coeffs_ref.shape
    per_leaf = 4 * 16
    stride = per_leaf + 8
    split_ref[...] = jnp.zeros_like(split_ref)
    parts = []
    for s in range(species):
        parts.append(coeffs_ref[s])
    both = jnp.concatenate(parts, axis=0)
    rest = both - both.astype(BF16).astype(F32)
    stacked = jnp.concatenate([both, rest], axis=0).astype(BF16)
    for k in range(DEG):
        wanted = table_ref[:, k * PAIR_ROWS : (k + 1) * PAIR_ROWS]
        rows = lax.broadcasted_iota(jnp.int32, (width, PAIR_ROWS), 0)
        pick = jnp.where(rows == wanted, 1.0, 0.0).astype(BF16)
        moved = jnp.dot(stacked, pick, preferred_element_type=F32)
        for h in range(2 * species):
            split_ref[pl.ds(h * 16 + k, leaves, stride=stride), :] = moved[h * leaves : (h + 1) * leaves]

    @pl.loop(0, leaves)
    def _(leaf):
        block = split_ref[pl.ds(pl.multiple_of(leaf * stride, 8), per_leaf), :]
        half = per_leaf // 2
        upper = jnp.concatenate([block[:half], jnp.zeros_like(block[:half])], axis=0)
        left_ref[leaf] = jnp.concatenate([block, upper], axis=1).astype(BF16)

    y_ref[...] = jnp.zeros_like(y_ref)
    z_ref[...] = jnp.zeros_like(z_ref)
    row = lax.broadcasted_iota(jnp.int32, (8, PB), 0)

    @pl.loop(0, request_ref.shape[1] // 8)
    def _(group):
        at = pl.ds(pl.multiple_of(group * 8, 8), 8)
        along_x = polynomials(request_ref[0, at, :])
        along_y = polynomials(request_ref[1, at, :])
        along_z = polynomials(request_ref[2, at, :])
        for k in range(DEG):
            x_ref[k * 8 : (k + 1) * 8] = along_x[k]
            y_ref[pl.ds(k, 8, stride=24), :] = along_y[k]
            z_ref[pl.ds(k, 8, stride=24), :] = along_z[k]
        for i in range(8):
            x_rows = [jnp.broadcast_to(x_ref[pl.ds(k * 8 + i, 1), :], (8, PB)) for k in range(DEG)]
            y_first = y_ref[i * 24 : i * 24 + 8]
            y_last = y_ref[i * 24 + 8 : i * 24 + 16]
            products = []
            for b in range(8):
                before = row < DEG - 8 - b
                turned = pltpu.roll(y_first, 7 - b, 0) if b < 7 else y_first
                x_late = x_rows[DEG - b] if b > 0 else x_rows[0]
                products.append(x_rows[b] * y_first)
                products.append(jnp.where(before, x_rows[b], x_late) * jnp.where(before, y_last, turned))
            high, low = high_low(jnp.concatenate(products, axis=0))
            right = jnp.concatenate([high, low], axis=0)
            leaf = index_ref[group * 8 + i]
            sums = jnp.dot(left_ref[leaf], right, preferred_element_type=F32)
            sums = sums[:32] + sums[32:]
            weight = z_ref[i * 24 : i * 24 + 16]
            for s in range(species):
                line = jnp.sum(sums[s * 16 : (s + 1) * 16] * weight, axis=0, keepdims=True)
                out_ref[pl.ds(group * 16 + i * 2 + s, 1), :] = line


def collect_kernel(place_ref, rows_ref, out_ref, line_ref):
    copies, species, leaves, nodes = out_ref.shape

    @pl.loop(0, leaves)
    def _(leaf):
        for m in range(BLOCKS):
            row = place_ref[leaf * BLOCKS + m]
            for s in range(species):
                at = (s * BLOCKS + m) * leaves + leaf
                line_ref[pl.ds(at, 1), :] = rows_ref[pl.ds(row * species + s, 1), :]

    for s in range(species):
        for m in range(BLOCKS):
            at = (s * BLOCKS + m) * leaves
            for c in range(copies):
                out_ref[c, s, :, m * PB : (m + 1) * PB] = line_ref[at : at + leaves]


def fit_kernel(
    part_ref, reaction_ref, values_ref, fit_ref, up_ref, ghosts_ref, first_ref, last_ref, equivalent_ref
):
    part = part_ref[0]
    all_species = values_ref.shape[0]
    species, leaves, width = ghosts_ref.shape
    reacted = []
    for s in range(species):
        row = part * species + s
        mixing = reaction_ref[row, 0] * values_ref[0]
        for r in range(1, all_species):
            mixing = mixing + reaction_ref[row, r] * values_ref[r]
        reacted.append(values_ref[row] + jnp.tanh(mixing))
    reacted = jnp.concatenate(reacted, axis=0)
    rows = species * leaves
    high = reacted.astype(BF16)
    stacked = jnp.concatenate([reacted, reacted - high.astype(F32)], axis=0).astype(BF16)
    fit_high, fit_low = high_low(fit_ref[...])
    first = jnp.dot(stacked, fit_high, preferred_element_type=F32)
    second = jnp.dot(high, fit_low, preferred_element_type=F32)
    ghosts = (first[:rows] + first[rows:] + second).astype(BF16)
    equivalent = jnp.dot(ghosts, up_ref[...], preferred_element_type=F32).astype(BF16)
    points = up_ref.shape[1]
    for s in range(species):
        here = ghosts[s * leaves : (s + 1) * leaves]
        ghosts_ref[s] = here
        first_ref[s] = here[:MARGIN]
        last_ref[s] = here[leaves - MARGIN :]
    copies, _, lanes = equivalent_ref.shape
    pieces = [equivalent[s * leaves : (s + 1) * leaves] for s in range(species)]
    pieces.append(jnp.zeros((leaves, lanes - species * points), BF16))
    line = jnp.concatenate(pieces, axis=1)
    for c in range(copies):
        equivalent_ref[c] = line


def update_kernel(
    segment_ref, core_ref, before_ref, ghosts_ref, after_ref, near_src_ref, near_op_ref, far_src_ref, new_seg_ref,
    near_mat_ref, mine_ref, other_ref, trans_ref, down_ref, out_ref, wide_ref,
):
    segment = segment_ref[0]
    core = core_ref[0]
    species, slots, width = out_ref.shape
    leaves = ghosts_ref.shape[1]
    span = leaves + 2 * MARGIN
    total_leaves = new_seg_ref.shape[1]
    near = near_src_ref.shape[0]
    operators = far_src_ref.shape[0]

    start = segment * leaves - MOVE
    window = jnp.clip(lax.shift_right_arithmetic(start, 7) * 128, 0, total_leaves - 256)
    window = pl.multiple_of(window, 128)
    lists = [ref[:, pl.ds(window, 256)] for ref in (near_src_ref, near_op_ref, far_src_ref)]
    lists.append(jnp.broadcast_to(new_seg_ref[:, pl.ds(window, 256)], (8, 256)))
    lists = jnp.concatenate(lists, axis=0)
    lists = pltpu.roll(lists, (window - start) & 255, 1)
    lists = lists[:, :128].T[:slots]
    source = lists[:, :near]
    kind = lists[:, near : 2 * near]
    far = lists[:, 2 * near : 2 * near + operators]
    target = start + lax.broadcasted_iota(jnp.int32, (slots, 1), 0)
    live = (target >= 0) & (target < total_leaves) & (lists[:, 2 * near + operators :][:, :1] == segment)

    offset = jnp.where(live & (source >= 0), source - (segment * leaves - MARGIN), -1)
    columns = lax.broadcasted_iota(jnp.int32, (slots, span), 1)
    weights = []
    for o in range(near_mat_ref.shape[0]):
        chosen = jnp.where(kind == o, offset, -1)
        weight = jnp.zeros((slots, span), F32)
        for q in range(source.shape[1]):
            weight = weight + jnp.where(chosen[:, q : q + 1] == columns, 1.0, 0.0)
        weights.append(weight)
    own = []
    around = []
    for s in range(species):
        wide_ref[s, 0:MARGIN, :] = before_ref[s].astype(F32)
        wide_ref[s, MARGIN : MARGIN + leaves, :] = ghosts_ref[s].astype(F32)
        wide_ref[s, MARGIN + leaves : span, :] = after_ref[s].astype(F32)
        own.append(wide_ref[s, MOVE : MOVE + slots, :])
        around.append(wide_ref[s].astype(BF16))
    total = jnp.concatenate(own, axis=0)
    rows = species * slots
    for o in range(near_mat_ref.shape[0]):
        weight = weights[o].astype(BF16)
        grouped = jnp.concatenate(
            [jnp.dot(weight, around[s], preferred_element_type=F32) for s in range(species)], axis=0
        )
        rest = grouped - grouped.astype(BF16).astype(F32)
        stacked = jnp.concatenate([grouped, rest], axis=0).astype(BF16)
        term = jnp.dot(stacked, near_mat_ref[o], preferred_element_type=F32)
        total = total + term[:rows] + term[rows:]

    far_segment = lax.shift_right_logical(far, 4)
    far_row = lax.shift_right_logical(far_segment, 1) * leaves + (far & 15)
    far_ok = live & (far >= 0)
    here = (far_segment & 1) == core
    mine_row = jnp.where(far_ok & here, far_row, -1)
    other_row = jnp.where(far_ok & jnp.logical_not(here), far_row, -1)
    held = mine_ref.shape[0]
    taken = None
    for row, table in ((mine_row, mine_ref), (other_row, other_ref)):
        column = jnp.concatenate([row[:, o : o + 1] for o in range(operators)], axis=0)
        ids = lax.broadcasted_iota(jnp.int32, (operators * slots, held), 1)
        pick = jnp.where(column == ids, 1.0, 0.0).astype(BF16)
        part = jnp.dot(pick, table[...], preferred_element_type=F32)
        taken = part if taken is None else taken + part
    points = trans_ref.shape[1]
    local = None
    for o in range(operators):
        lines = taken[o * slots : (o + 1) * slots]
        both = jnp.concatenate([lines[:, s * points : (s + 1) * points] for s in range(species)], axis=0)
        term = jnp.dot(both.astype(BF16), trans_ref[o], preferred_element_type=F32)
        local = term if local is None else local + term
    total = total + jnp.dot(local.astype(BF16), down_ref[...], preferred_element_type=F32)
    for s in range(species):
        out_ref[s] = jnp.where(live, total[s * slots : (s + 1) * slots], 0.0)


def spaces(text):
    names = {"s": pltpu.SMEM, "v": pltpu.VMEM}
    return [pl.BlockSpec(memory_space=names[c]) for c in text]


def within(mebibytes):
    return pltpu.CompilerParams(vmem_limit_bytes=mebibytes * 1024 * 1024)


def shards(
    coeffs, points, owner_leaf, reaction, fit_matrix, new_seg, near_src, near_op, near_mat, up_mat,
    far_src, trans_mat, down_mat,
):
    species, leaves, width = coeffs.shape
    segments = lax.axis_size(SEG)
    segment = lax.axis_index(SEG)
    part = lax.axis_index("sp")
    parts = lax.axis_size("sp")
    part_id = jnp.full((1,), part, jnp.int32)
    slots = segments * CAP
    shape = jax.ShapeDtypeStruct

    request, place = pl.pallas_call(
        route_kernel,
        out_shape=(shape((slots, PB), F32), shape((leaves * BLOCKS,), jnp.int32)),
        in_specs=spaces("ssv"),
        out_specs=tuple(spaces("vs")),
        scratch_shapes=[pltpu.SMEM((segments,), jnp.int32), pltpu.VMEM((leaves * BLOCKS, PB), F32)],
        compiler_params=within(4),
    )(part_id, owner_leaf, points)
    request = lax.all_to_all(request.reshape(segments, CAP, PB), SEG, 0, 0, tiled=True)
    request = jnp.broadcast_to(request.reshape(1, slots, PB), (parts, slots, PB))
    request = lax.all_to_all(request, "sp", 0, 0, tiled=True)
    index = jnp.clip(request[3, :, 0].astype(jnp.int32), 0, leaves - 1)
    answers = pl.pallas_call(
        evaluate_kernel,
        out_shape=shape((slots * species, PB), F32),
        in_specs=spaces("svvv"),
        out_specs=spaces("v")[0],
        scratch_shapes=[
            pltpu.VMEM((leaves * 72, PB), F32),
            pltpu.VMEM((leaves, 64, 2 * PB), BF16),
            pltpu.VMEM((DEG * 8, PB), F32),
            pltpu.VMEM((8 * 24, PB), F32),
            pltpu.VMEM((8 * 24, PB), F32),
        ],
        compiler_params=within(16),
    )(index, request, coeffs, jnp.asarray(coefficient_table()))
    answers = lax.all_to_all(answers.reshape(segments, CAP * species, PB), SEG, 0, 0, tiled=True)
    values = pl.pallas_call(
        collect_kernel,
        out_shape=shape((parts, species, leaves, BLOCKS * PB), F32),
        in_specs=spaces("sv"),
        out_specs=spaces("v")[0],
        scratch_shapes=[pltpu.VMEM((species * leaves * BLOCKS, PB), F32)],
        compiler_params=within(4),
    )(place, answers.reshape(slots * species, PB))
    gathered = lax.all_to_all(values, "sp", 0, 0, tiled=True).reshape(parts * species, leaves, BLOCKS * PB)
    z_size = lax.axis_size("seg_1")
    edge = shape((species, MARGIN, width), BF16)
    ghosts, first, last, spread = pl.pallas_call(
        fit_kernel,
        out_shape=(shape((species, leaves, width), BF16), edge, edge, shape((z_size, leaves, LANES), BF16)),
        in_specs=spaces("ssvvv"),
        out_specs=tuple(spaces("vvvv")),
        compiler_params=within(24),
    )(part_id, reaction, gathered, fit_matrix, up_mat)

    up = [(i, i + 1) for i in range(segments - 1)]
    down = [(j, i) for i, j in up]
    before = lax.ppermute(last, SEG, up)
    after = lax.ppermute(first, SEG, down)
    along_z = lax.all_to_all(spread, "seg_1", 0, 0, tiled=True)
    mine = lax.all_gather(along_z.reshape(z_size * leaves, LANES), "seg_0", axis=0, tiled=True)
    other = lax.ppermute(mine, "seg_2", [(0, 1), (1, 0)])

    slot_total = leaves + 2 * MOVE
    return pl.pallas_call(
        update_kernel,
        out_shape=shape((species, slot_total, width), F32),
        in_specs=spaces("ssvvvvvvvvvvvv"),
        out_specs=spaces("v")[0],
        scratch_shapes=[pltpu.VMEM((species, leaves + 2 * MARGIN, width), F32)],
        compiler_params=within(24),
    )(
        jnp.full((1,), segment, jnp.int32), jnp.full((1,), lax.axis_index("seg_2"), jnp.int32),
        before, ghosts, after, near_src.T, near_op.T, far_src.T, new_seg.reshape(1, -1),
        near_mat, mine, other, trans_mat, down_mat,
    )


def solution(mesh):
    torus = Mesh(
        mesh.devices.reshape(4, 16, 2, mesh.shape["sp"]), ("seg_0", "seg_1", "seg_2", "sp")
    )
    whole = P()
    return jax.shard_map(
        shards,
        mesh=torus,
        in_specs=(P("sp", SEG, None), P(None, SEG, None), P(SEG, None)) + (whole,) * 10,
        out_specs=P("sp", SEG, None),
        check_vma=False,
    )
```

```python
import functools

import jax
import jax.numpy as jnp
import numpy as np
from jax import lax
from jax.experimental import pallas as pl
from jax.experimental.pallas import tpu as pltpu
from jax.sharding import Mesh
from jax.sharding import PartitionSpec as P


ORDER = 14
DEG = ORDER + 1
BLOCKS = 6
PB = 128
MOVE = 4
REACH = 4
MARGIN = MOVE + REACH
CAP = 2
PAIR_ROWS = 128
LANES = 384
SEG = ("seg_0", "seg_1", "seg_2")
F32 = jnp.float32
BF16 = jnp.bfloat16


def degree_pairs():
    pairs = []
    for i in range(8):
        for r in range(16):
            pairs.append((i, r) if r < DEG - i else (DEG - i, r - (DEG - i)))
    return pairs


def coefficient_table():
    number = {}
    for i in range(DEG):
        for j in range(DEG - i):
            for k in range(DEG - i - j):
                number[i, j, k] = len(number)
    table = np.full((DEG, PAIR_ROWS), -1, np.int32)
    for k in range(DEG):
        for q, (i, j) in enumerate(degree_pairs()):
            if i + j + k <= ORDER:
                table[k, q] = number[i, j, k]
    return table.reshape(1, DEG * PAIR_ROWS)


def high_low(value):
    high = value.astype(BF16)
    return high, (value - high.astype(F32)).astype(BF16)


def polynomials(x):
    terms = [jnp.ones_like(x), x]
    for _ in range(2, DEG):
        terms.append(2.0 * x * terms[-1] - terms[-2])
    return terms


def route_kernel(
    part_ref, owner_hbm, points_ref, request_ref, place_ref, count_ref, owner_ref, plane_ref, line_ref, sem, owner_sem
):
    part = part_ref[0]
    owners = pltpu.make_async_copy(owner_hbm, owner_ref, owner_sem)
    owners.start()
    blocks, leaves = owner_ref.shape
    fetch = pltpu.make_async_copy(points_ref.at[jnp.minimum(part, 2)], plane_ref, sem)
    fetch.start()
    request_ref[...] = jnp.zeros_like(request_ref)

    @pl.loop(0, count_ref.shape[0] // 8)
    def _(d):
        for i in range(8):
            count_ref[d * 8 + i] = 0

    owners.wait()

    @pl.loop(0, leaves)
    def _(leaf):
        for m in range(blocks):
            target = lax.shift_right_logical(owner_ref[m, leaf], 4)
            used = count_ref[target]
            count_ref[target] = used + 1
            place_ref[leaf * blocks + m] = target * CAP + used

    fetch.wait()
    for m in range(blocks):
        line_ref[m * leaves : (m + 1) * leaves] = plane_ref[:, m * PB : (m + 1) * PB]

    @pl.loop(0, leaves)
    def _(leaf):
        for m in range(blocks):
            line = line_ref[pl.ds(m * leaves + leaf, 1), :]
            index = jnp.full((1, PB), (owner_ref[m, leaf] & 15).astype(F32), F32)
            request_ref[pl.ds(place_ref[leaf * blocks + m], 1), :] = jnp.where(part == 3, index, line)


def evaluate_kernel(index_ref, request_ref, coeffs_ref, table_ref, out_ref, split_ref, left_ref, x_ref, y_ref, z_ref):
    species, leaves, width = coeffs_ref.shape
    per_leaf = 4 * 16
    stride = per_leaf + 8
    split_ref[...] = jnp.zeros_like(split_ref)
    parts = []
    for s in range(species):
        parts.append(coeffs_ref[s])
    both = jnp.concatenate(parts, axis=0)
    rest = both - both.astype(BF16).astype(F32)
    stacked = jnp.concatenate([both, rest], axis=0).astype(BF16)
    for k in range(DEG):
        wanted = table_ref[:, k * PAIR_ROWS : (k + 1) * PAIR_ROWS]
        rows = lax.broadcasted_iota(jnp.int32, (width, PAIR_ROWS), 0)
        pick = jnp.where(rows == wanted, 1.0, 0.0).astype(BF16)
        moved = jnp.dot(stacked, pick, preferred_element_type=F32)
        for h in range(2 * species):
            split_ref[pl.ds(h * 16 + k, leaves, stride=stride), :] = moved[h * leaves : (h + 1) * leaves]

    @pl.loop(0, leaves)
    def _(leaf):
        block = split_ref[pl.ds(pl.multiple_of(leaf * stride, 8), per_leaf), :]
        half = per_leaf // 2
        upper = jnp.concatenate([block[:half], jnp.zeros_like(block[:half])], axis=0)
        left_ref[leaf] = jnp.concatenate([block, upper], axis=1).astype(BF16)

    y_ref[...] = jnp.zeros_like(y_ref)
    z_ref[...] = jnp.zeros_like(z_ref)
    row = lax.broadcasted_iota(jnp.int32, (8, PB), 0)

    @pl.loop(0, request_ref.shape[1] // 8)
    def _(group):
        at = pl.ds(pl.multiple_of(group * 8, 8), 8)
        along_x = polynomials(request_ref[0, at, :])
        along_y = polynomials(request_ref[1, at, :])
        along_z = polynomials(request_ref[2, at, :])
        for k in range(DEG):
            x_ref[k * 8 : (k + 1) * 8] = along_x[k]
            y_ref[pl.ds(k, 8, stride=24), :] = along_y[k]
            z_ref[pl.ds(k, 8, stride=24), :] = along_z[k]
        for i in range(8):
            x_rows = [jnp.broadcast_to(x_ref[pl.ds(k * 8 + i, 1), :], (8, PB)) for k in range(DEG)]
            y_first = y_ref[i * 24 : i * 24 + 8]
            y_last = y_ref[i * 24 + 8 : i * 24 + 16]
            products = []
            for b in range(8):
                before = row < DEG - 8 - b
                turned = pltpu.roll(y_first, 7 - b, 0) if b < 7 else y_first
                x_late = x_rows[DEG - b] if b > 0 else x_rows[0]
                products.append(x_rows[b] * y_first)
                products.append(jnp.where(before, x_rows[b], x_late) * jnp.where(before, y_last, turned))
            high, low = high_low(jnp.concatenate(products, axis=0))
            right = jnp.concatenate([high, low], axis=0)
            leaf = index_ref[group * 8 + i]
            sums = jnp.dot(left_ref[leaf], right, preferred_element_type=F32)
            sums = sums[:32] + sums[32:]
            weight = z_ref[i * 24 : i * 24 + 16]
            for s in range(species):
                line = jnp.sum(sums[s * 16 : (s + 1) * 16] * weight, axis=0, keepdims=True)
                out_ref[pl.ds(group * 16 + i * 2 + s, 1), :] = line


def collect_kernel(place_ref, rows_ref, out_ref, line_ref):
    copies, species, leaves, _ = out_ref.shape

    @pl.loop(0, leaves)
    def _(leaf):
        for m in range(BLOCKS):
            row = place_ref[leaf * BLOCKS + m]
            for s in range(species):
                at = (s * BLOCKS + m) * leaves + leaf
                line_ref[pl.ds(at, 1), :] = rows_ref[pl.ds(row * species + s, 1), :]

    for s in range(species):
        for m in range(BLOCKS):
            at = (s * BLOCKS + m) * leaves
            for c in range(copies):
                out_ref[c, s, :, m * PB : (m + 1) * PB] = line_ref[at : at + leaves]


def fit_kernel(
    part_ref, segment_ref, reaction_ref, values_ref, fit_ref, up_ref, near_src_ref, near_op_ref, far_src_ref,
    new_seg_ref, ghosts_ref, first_ref, last_ref, equivalent_ref, lists_ref, window_ref, owned_ref, sems,
):
    part = part_ref[0]
    start = segment_ref[0] * ghosts_ref.shape[1] - MOVE
    window = jnp.clip(lax.shift_right_arithmetic(start, 7) * 128, 0, new_seg_ref.shape[1] - 256)
    window = pl.multiple_of(window, 128)
    fetches = []
    at = 0
    for n, ref in enumerate((near_src_ref, near_op_ref, far_src_ref, new_seg_ref)):
        held = window_ref.at[pl.ds(at, ref.shape[0])] if n < 3 else owned_ref
        fetches.append(pltpu.make_async_copy(ref.at[:, pl.ds(window, 256)], held, sems.at[n]))
        fetches[-1].start()
        at += ref.shape[0]
    all_species = values_ref.shape[0]
    species, leaves, _ = ghosts_ref.shape
    reacted = []
    for s in range(species):
        row = part * species + s
        mixing = reaction_ref[row, 0] * values_ref[0]
        for r in range(1, all_species):
            mixing = mixing + reaction_ref[row, r] * values_ref[r]
        reacted.append(values_ref[row] + jnp.tanh(mixing))
    reacted = jnp.concatenate(reacted, axis=0)
    rows = species * leaves
    high = reacted.astype(BF16)
    stacked = jnp.concatenate([reacted, reacted - high.astype(F32)], axis=0).astype(BF16)
    fit_high, fit_low = high_low(fit_ref[...])
    first = jnp.dot(stacked, fit_high, preferred_element_type=F32)
    second = jnp.dot(high, fit_low, preferred_element_type=F32)
    ghosts = (first[:rows] + first[rows:] + second).astype(BF16)
    equivalent = jnp.dot(ghosts, up_ref[...], preferred_element_type=F32).astype(BF16)
    points = up_ref.shape[1]
    for s in range(species):
        here = ghosts[s * leaves : (s + 1) * leaves]
        ghosts_ref[s] = here
        first_ref[s] = here[:MARGIN]
        last_ref[s] = here[leaves - MARGIN :]
    copies, _, lanes = equivalent_ref.shape
    pieces = [equivalent[s * leaves : (s + 1) * leaves] for s in range(species)]
    pieces.append(jnp.zeros((leaves, lanes - species * points), BF16))
    line = jnp.concatenate(pieces, axis=1)
    for c in range(copies):
        equivalent_ref[c] = line
    for fetch in fetches:
        fetch.wait()
    lists = jnp.concatenate([window_ref[...], jnp.broadcast_to(owned_ref[...], (8, 256))], axis=0)
    lists = pltpu.roll(lists, (window - start) & 255, 1)
    lists_ref[...] = lists[:, :128].T[: lists_ref.shape[0]]


def update_kernel(
    total_leaves, near, segment_ref, core_ref, before_ref, ghosts_ref, after_ref, lists_ref, near_mat_hbm, mine_ref,
    other_ref, trans_hbm, down_hbm, out_ref, wide_ref, near_mat_ref, trans_ref, down_ref, sems,
):
    segment = segment_ref[0]
    core = core_ref[0]
    species, slots, _ = out_ref.shape
    leaves = ghosts_ref.shape[1]
    span = leaves + 2 * MARGIN
    operators = trans_ref.shape[0]
    fetches = []
    for n, (ref, held) in enumerate(
        ((trans_hbm, trans_ref), (down_hbm, down_ref), (near_mat_hbm, near_mat_ref))
    ):
        fetches.append(pltpu.make_async_copy(ref, held, sems.at[n]))
        fetches[-1].start()
    start = segment * leaves - MOVE
    lists = lists_ref[...]
    source = lists[:, :near]
    kind = lists[:, near : 2 * near]
    far = lists[:, 2 * near : 2 * near + operators]
    target = start + lax.broadcasted_iota(jnp.int32, (slots, 1), 0)
    live = (target >= 0) & (target < total_leaves) & (lists[:, 2 * near + operators : 2 * near + operators + 1] == segment)

    far_segment = lax.shift_right_logical(far, 4)
    far_row = lax.shift_right_logical(far_segment, 1) * leaves + (far & 15)
    far_ok = live & (far >= 0)
    here = (far_segment & 1) == core
    mine_row = jnp.where(far_ok & here, far_row, -1)
    other_row = jnp.where(far_ok & jnp.logical_not(here), far_row, -1)
    held = mine_ref.shape[0]
    taken = None
    for row, table in ((mine_row, mine_ref), (other_row, other_ref)):
        column = jnp.concatenate([row[:, o : o + 1] for o in range(operators)], axis=0)
        ids = lax.broadcasted_iota(jnp.int32, (operators * slots, held), 1)
        pick = jnp.where(column == ids, 1.0, 0.0).astype(BF16)
        part = jnp.dot(pick, table[...], preferred_element_type=F32)
        taken = part if taken is None else taken + part
    points = trans_ref.shape[1]
    fetches[0].wait()
    local = None
    for o in range(operators):
        lines = taken[o * slots : (o + 1) * slots]
        both = jnp.concatenate([lines[:, s * points : (s + 1) * points] for s in range(species)], axis=0)
        term = jnp.dot(both.astype(BF16), trans_ref[o], preferred_element_type=F32)
        local = term if local is None else local + term
    fetches[1].wait()
    total = jnp.dot(local.astype(BF16), down_ref[...], preferred_element_type=F32)

    offset = jnp.where(live & (source >= 0), source - (segment * leaves - MARGIN), -1)
    columns = lax.broadcasted_iota(jnp.int32, (slots, span), 1)
    weights = []
    for o in range(near_mat_ref.shape[0]):
        chosen = jnp.where(kind == o, offset, -1)
        weight = jnp.zeros((slots, span), F32)
        for q in range(source.shape[1]):
            weight = weight + jnp.where(chosen[:, q : q + 1] == columns, 1.0, 0.0)
        weights.append(weight)
    own = []
    around = []
    for s in range(species):
        wide_ref[s, 0:MARGIN, :] = before_ref[s].astype(F32)
        wide_ref[s, MARGIN : MARGIN + leaves, :] = ghosts_ref[s].astype(F32)
        wide_ref[s, MARGIN + leaves : span, :] = after_ref[s].astype(F32)
        own.append(wide_ref[s, MOVE : MOVE + slots, :])
        around.append(wide_ref[s].astype(BF16))
    total = total + jnp.concatenate(own, axis=0)
    rows = species * slots
    fetches[2].wait()
    for o in range(near_mat_ref.shape[0]):
        weight = weights[o].astype(BF16)
        grouped = jnp.concatenate(
            [jnp.dot(weight, around[s], preferred_element_type=F32) for s in range(species)], axis=0
        )
        rest = grouped - grouped.astype(BF16).astype(F32)
        stacked = jnp.concatenate([grouped, rest], axis=0).astype(BF16)
        term = jnp.dot(stacked, near_mat_ref[o], preferred_element_type=F32)
        total = total + term[:rows] + term[rows:]

    for s in range(species):
        out_ref[s] = jnp.where(live, total[s * slots : (s + 1) * slots], 0.0)


def spaces(text):
    names = {"s": pltpu.SMEM, "v": pltpu.VMEM, "h": pltpu.HBM}
    return [pl.BlockSpec(memory_space=names[c]) for c in text]


def within(mebibytes):
    return pltpu.CompilerParams(vmem_limit_bytes=mebibytes * 1024 * 1024)


def shards(
    coeffs, points, owner_leaf, reaction, fit_matrix, new_seg, near_src, near_op, near_mat, up_mat,
    far_src, trans_mat, down_mat,
):
    species, leaves, width = coeffs.shape
    segments = lax.axis_size(SEG)
    segment = lax.axis_index(SEG)
    part = lax.axis_index("sp")
    parts = lax.axis_size("sp")
    part_id = jnp.full((1,), part, jnp.int32)
    segment_id = jnp.full((1,), segment, jnp.int32)
    slots = segments * CAP
    shape = jax.ShapeDtypeStruct

    request, place = pl.pallas_call(
        route_kernel,
        out_shape=(shape((slots, PB), F32), shape((leaves * BLOCKS,), jnp.int32)),
        in_specs=spaces("shh"),
        out_specs=tuple(spaces("vs")),
        scratch_shapes=[
            pltpu.SMEM((segments,), jnp.int32),
            pltpu.SMEM((BLOCKS, leaves), jnp.int32),
            pltpu.VMEM((leaves, BLOCKS * PB), F32),
            pltpu.VMEM((leaves * BLOCKS, PB), F32),
            pltpu.SemaphoreType.DMA,
            pltpu.SemaphoreType.DMA,
        ],
        compiler_params=within(4),
    )(part_id, owner_leaf.T, points)
    request = lax.all_to_all(request.reshape(segments, CAP, PB), SEG, 0, 0, tiled=True)
    request = jnp.broadcast_to(request.reshape(1, slots, PB), (parts, slots, PB))
    request = lax.all_to_all(request, "sp", 0, 0, tiled=True)
    index = jnp.clip(request[3, :, 0].astype(jnp.int32), 0, leaves - 1)
    answers = pl.pallas_call(
        evaluate_kernel,
        out_shape=shape((slots * species, PB), F32),
        in_specs=spaces("svvv"),
        out_specs=spaces("v")[0],
        scratch_shapes=[
            pltpu.VMEM((leaves * 72, PB), F32),
            pltpu.VMEM((leaves, 64, 2 * PB), BF16),
            pltpu.VMEM((DEG * 8, PB), F32),
            pltpu.VMEM((8 * 24, PB), F32),
            pltpu.VMEM((8 * 24, PB), F32),
        ],
        compiler_params=within(16),
    )(index, request, coeffs, jnp.asarray(coefficient_table()))
    answers = lax.all_to_all(answers.reshape(segments, CAP * species, PB), SEG, 0, 0, tiled=True)
    values = pl.pallas_call(
        collect_kernel,
        out_shape=shape((parts, species, leaves, BLOCKS * PB), F32),
        in_specs=spaces("sv"),
        out_specs=spaces("v")[0],
        scratch_shapes=[pltpu.VMEM((species * leaves * BLOCKS, PB), F32)],
        compiler_params=within(4),
    )(place, answers.reshape(slots * species, PB))
    gathered = lax.all_to_all(values, "sp", 0, 0, tiled=True).reshape(parts * species, leaves, BLOCKS * PB)
    z_size = lax.axis_size("seg_1")
    edge = shape((species, MARGIN, width), BF16)
    slot_total = leaves + 2 * MOVE
    near = near_src.shape[1]
    listed = 2 * near + far_src.shape[1] + 8
    ghosts, first, last, spread, lists = pl.pallas_call(
        fit_kernel,
        out_shape=(
            shape((species, leaves, width), BF16), edge, edge, shape((z_size, leaves, LANES), BF16),
            shape((slot_total, listed), jnp.int32),
        ),
        in_specs=spaces("sssvvvhhhh"),
        out_specs=tuple(spaces("vvvvv")),
        scratch_shapes=[
            pltpu.VMEM((listed - 8, 256), jnp.int32), pltpu.VMEM((1, 256), jnp.int32), pltpu.SemaphoreType.DMA((4,)),
        ],
        compiler_params=within(24),
    )(
        part_id, segment_id, reaction, gathered, fit_matrix, up_mat, near_src.T, near_op.T, far_src.T,
        new_seg.reshape(1, -1),
    )

    up = [(i, i + 1) for i in range(segments - 1)]
    down = [(j, i) for i, j in up]
    before = lax.ppermute(last, SEG, up)
    after = lax.ppermute(first, SEG, down)
    along_z = lax.all_to_all(spread, "seg_1", 0, 0, tiled=True)
    mine = lax.all_gather(along_z.reshape(z_size * leaves, LANES), "seg_0", axis=0, tiled=True)
    other = lax.ppermute(mine, "seg_2", [(0, 1), (1, 0)])

    return pl.pallas_call(
        functools.partial(update_kernel, new_seg.shape[0], near),
        out_shape=shape((species, slot_total, width), F32),
        in_specs=spaces("ssvvvvhvvhh"),
        out_specs=spaces("v")[0],
        scratch_shapes=[
            pltpu.VMEM((species, leaves + 2 * MARGIN, width), F32),
            pltpu.VMEM(near_mat.shape, BF16),
            pltpu.VMEM(trans_mat.shape, BF16),
            pltpu.VMEM(down_mat.shape, BF16),
            pltpu.SemaphoreType.DMA((3,)),
        ],
        compiler_params=within(24),
    )(
        segment_id, jnp.full((1,), lax.axis_index("seg_2"), jnp.int32), before, ghosts, after, lists, near_mat, mine,
        other, trans_mat, down_mat,
    )


def solution(mesh):
    torus = Mesh(
        mesh.devices.reshape(4, 16, 2, mesh.shape["sp"]), ("seg_0", "seg_1", "seg_2", "sp")
    )
    whole = P()
    return jax.shard_map(
        shards,
        mesh=torus,
        in_specs=(P("sp", SEG, None), P(None, SEG, None), P(SEG, None)) + (whole,) * 10,
        out_specs=P("sp", SEG, None),
        check_vma=False,
    )
```

```python
import functools

import jax
import jax.numpy as jnp
import numpy as np
from jax import lax
from jax.experimental import pallas as pl
from jax.experimental.pallas import tpu as pltpu
from jax.sharding import Mesh
from jax.sharding import PartitionSpec as P


ORDER = 14
DEG = ORDER + 1
BLOCKS = 6
PB = 128
MOVE = 4
REACH = 4
MARGIN = MOVE + REACH
CAP = 2
PAIR_ROWS = 128
LANES = 384
SEG = ("seg_0", "seg_1", "seg_2")
F32 = jnp.float32
BF16 = jnp.bfloat16


def degree_pairs():
    pairs = []
    for i in range(8):
        for r in range(16):
            pairs.append((i, r) if r < DEG - i else (DEG - i, r - (DEG - i)))
    return pairs


def coefficient_table():
    number = {}
    for i in range(DEG):
        for j in range(DEG - i):
            for k in range(DEG - i - j):
                number[i, j, k] = len(number)
    table = np.full((DEG, PAIR_ROWS), -1, np.int32)
    for k in range(DEG):
        for q, (i, j) in enumerate(degree_pairs()):
            if i + j + k <= ORDER:
                table[k, q] = number[i, j, k]
    return table.reshape(1, DEG * PAIR_ROWS)


def high_low(value):
    high = value.astype(BF16)
    return high, (value - high.astype(F32)).astype(BF16)


def polynomials(x):
    terms = [jnp.ones_like(x), x]
    for _ in range(2, DEG):
        terms.append(2.0 * x * terms[-1] - terms[-2])
    return terms


def route_kernel(
    part_ref, owner_hbm, points_ref, request_ref, place_ref, count_ref, owner_ref, plane_ref, line_ref, sem, owner_sem
):
    part = part_ref[0]
    owners = pltpu.make_async_copy(owner_hbm, owner_ref, owner_sem)
    owners.start()
    blocks, leaves = owner_ref.shape
    fetch = pltpu.make_async_copy(points_ref.at[jnp.minimum(part, 2)], plane_ref, sem)
    fetch.start()
    request_ref[...] = jnp.zeros_like(request_ref)

    @pl.loop(0, count_ref.shape[0] // 8)
    def _(d):
        for i in range(8):
            count_ref[d * 8 + i] = 0

    owners.wait()

    @pl.loop(0, leaves)
    def _(leaf):
        for m in range(blocks):
            target = lax.shift_right_logical(owner_ref[m, leaf], 4)
            used = count_ref[target]
            count_ref[target] = used + 1
            place_ref[leaf * blocks + m] = target * CAP + used

    fetch.wait()
    for m in range(blocks):
        line_ref[m * leaves : (m + 1) * leaves] = plane_ref[:, m * PB : (m + 1) * PB]

    @pl.loop(0, leaves)
    def _(leaf):
        for m in range(blocks):
            line = line_ref[pl.ds(m * leaves + leaf, 1), :]
            index = jnp.full((1, PB), (owner_ref[m, leaf] & 15).astype(F32), F32)
            request_ref[pl.ds(place_ref[leaf * blocks + m], 1), :] = jnp.where(part == 3, index, line)


def arrange_kernel(coeffs_ref, table_ref, left_ref, split_ref):
    species, leaves, width = coeffs_ref.shape
    per_leaf = 4 * 16
    stride = per_leaf + 8
    split_ref[...] = jnp.zeros_like(split_ref)
    both = jnp.concatenate([coeffs_ref[s] for s in range(species)], axis=0)
    rest = both - both.astype(BF16).astype(F32)
    stacked = jnp.concatenate([both, rest], axis=0).astype(BF16)
    for k in range(DEG):
        wanted = table_ref[:, k * PAIR_ROWS : (k + 1) * PAIR_ROWS]
        rows = lax.broadcasted_iota(jnp.int32, (width, PAIR_ROWS), 0)
        pick = jnp.where(rows == wanted, 1.0, 0.0).astype(BF16)
        moved = jnp.dot(stacked, pick, preferred_element_type=F32)
        for h in range(2 * species):
            split_ref[pl.ds(h * 16 + k, leaves, stride=stride), :] = moved[h * leaves : (h + 1) * leaves]

    @pl.loop(0, leaves)
    def _(leaf):
        block = split_ref[pl.ds(pl.multiple_of(leaf * stride, 8), per_leaf), :]
        half = per_leaf // 2
        upper = jnp.concatenate([block[:half], jnp.zeros_like(block[:half])], axis=0)
        left_ref[leaf] = jnp.concatenate([block, upper], axis=1).astype(BF16)


def evaluate_kernel(species, index_ref, request_ref, left_ref, out_ref, x_ref, y_ref, z_ref):
    y_ref[...] = jnp.zeros_like(y_ref)
    z_ref[...] = jnp.zeros_like(z_ref)
    row = lax.broadcasted_iota(jnp.int32, (8, PB), 0)

    @pl.loop(0, request_ref.shape[1] // 8)
    def _(group):
        at = pl.ds(pl.multiple_of(group * 8, 8), 8)
        along_x = polynomials(request_ref[0, at, :])
        along_y = polynomials(request_ref[1, at, :])
        along_z = polynomials(request_ref[2, at, :])
        for k in range(DEG):
            x_ref[k * 8 : (k + 1) * 8] = along_x[k]
            y_ref[pl.ds(k, 8, stride=24), :] = along_y[k]
            z_ref[pl.ds(k, 8, stride=24), :] = along_z[k]
        for i in range(8):
            x_rows = [jnp.broadcast_to(x_ref[pl.ds(k * 8 + i, 1), :], (8, PB)) for k in range(DEG)]
            y_first = y_ref[i * 24 : i * 24 + 8]
            y_last = y_ref[i * 24 + 8 : i * 24 + 16]
            products = []
            for b in range(8):
                before = row < DEG - 8 - b
                turned = pltpu.roll(y_first, 7 - b, 0) if b < 7 else y_first
                x_late = x_rows[DEG - b] if b > 0 else x_rows[0]
                products.append(x_rows[b] * y_first)
                products.append(jnp.where(before, x_rows[b], x_late) * jnp.where(before, y_last, turned))
            high, low = high_low(jnp.concatenate(products, axis=0))
            right = jnp.concatenate([high, low], axis=0)
            leaf = index_ref[group * 8 + i]
            sums = jnp.dot(left_ref[leaf], right, preferred_element_type=F32)
            sums = sums[:32] + sums[32:]
            weight = z_ref[i * 24 : i * 24 + 16]
            for s in range(species):
                line = jnp.sum(sums[s * 16 : (s + 1) * 16] * weight, axis=0, keepdims=True)
                out_ref[pl.ds(group * 16 + i * 2 + s, 1), :] = line


def collect_kernel(place_ref, rows_ref, out_ref, line_ref):
    copies, species, leaves, _ = out_ref.shape

    @pl.loop(0, leaves)
    def _(leaf):
        for m in range(BLOCKS):
            row = place_ref[leaf * BLOCKS + m]
            for s in range(species):
                at = (s * BLOCKS + m) * leaves + leaf
                line_ref[pl.ds(at, 1), :] = rows_ref[pl.ds(row * species + s, 1), :]

    for s in range(species):
        for m in range(BLOCKS):
            at = (s * BLOCKS + m) * leaves
            for c in range(copies):
                out_ref[c, s, :, m * PB : (m + 1) * PB] = line_ref[at : at + leaves]


def fit_kernel(
    part_ref, segment_ref, reaction_ref, values_ref, fit_ref, up_ref, near_src_ref, near_op_ref, far_src_ref,
    new_seg_ref, ghosts_ref, first_ref, last_ref, equivalent_ref, lists_ref, window_ref, owned_ref, sems,
):
    part = part_ref[0]
    start = segment_ref[0] * ghosts_ref.shape[1] - MOVE
    window = jnp.clip(lax.shift_right_arithmetic(start, 7) * 128, 0, new_seg_ref.shape[1] - 256)
    window = pl.multiple_of(window, 128)
    fetches = []
    at = 0
    for n, ref in enumerate((near_src_ref, near_op_ref, far_src_ref, new_seg_ref)):
        held = window_ref.at[pl.ds(at, ref.shape[0])] if n < 3 else owned_ref
        fetches.append(pltpu.make_async_copy(ref.at[:, pl.ds(window, 256)], held, sems.at[n]))
        fetches[-1].start()
        at += ref.shape[0]
    all_species = values_ref.shape[0]
    species, leaves, _ = ghosts_ref.shape
    reacted = []
    for s in range(species):
        row = part * species + s
        mixing = reaction_ref[row, 0] * values_ref[0]
        for r in range(1, all_species):
            mixing = mixing + reaction_ref[row, r] * values_ref[r]
        reacted.append(values_ref[row] + jnp.tanh(mixing))
    reacted = jnp.concatenate(reacted, axis=0)
    rows = species * leaves
    high = reacted.astype(BF16)
    stacked = jnp.concatenate([reacted, reacted - high.astype(F32)], axis=0).astype(BF16)
    fit_high, fit_low = high_low(fit_ref[...])
    first = jnp.dot(stacked, fit_high, preferred_element_type=F32)
    second = jnp.dot(high, fit_low, preferred_element_type=F32)
    ghosts = (first[:rows] + first[rows:] + second).astype(BF16)
    equivalent = jnp.dot(ghosts, up_ref[...], preferred_element_type=F32).astype(BF16)
    points = up_ref.shape[1]
    for s in range(species):
        here = ghosts[s * leaves : (s + 1) * leaves]
        ghosts_ref[s] = here
        first_ref[s] = here[:MARGIN]
        last_ref[s] = here[leaves - MARGIN :]
    copies, _, lanes = equivalent_ref.shape
    pieces = [equivalent[s * leaves : (s + 1) * leaves] for s in range(species)]
    pieces.append(jnp.zeros((leaves, lanes - species * points), BF16))
    line = jnp.concatenate(pieces, axis=1)
    for c in range(copies):
        equivalent_ref[c] = line
    for fetch in fetches:
        fetch.wait()
    lists = jnp.concatenate([window_ref[...], jnp.broadcast_to(owned_ref[...], (8, 256))], axis=0)
    lists = pltpu.roll(lists, (window - start) & 255, 1)
    lists_ref[...] = lists[:, :128].T[: lists_ref.shape[0]]


def update_kernel(
    total_leaves, near, segment_ref, core_ref, before_ref, ghosts_ref, after_ref, lists_ref, near_mat_ref, mine_ref,
    other_ref, trans_ref, down_ref, out_ref, wide_ref,
):
    segment = segment_ref[0]
    core = core_ref[0]
    species, slots, _ = out_ref.shape
    leaves = ghosts_ref.shape[1]
    span = leaves + 2 * MARGIN
    operators = trans_ref.shape[0]
    start = segment * leaves - MOVE
    lists = lists_ref[...]
    source = lists[:, :near]
    kind = lists[:, near : 2 * near]
    far = lists[:, 2 * near : 2 * near + operators]
    target = start + lax.broadcasted_iota(jnp.int32, (slots, 1), 0)
    live = (target >= 0) & (target < total_leaves) & (lists[:, 2 * near + operators : 2 * near + operators + 1] == segment)

    far_segment = lax.shift_right_logical(far, 4)
    far_row = lax.shift_right_logical(far_segment, 1) * leaves + (far & 15)
    far_ok = live & (far >= 0)
    here = (far_segment & 1) == core
    mine_row = jnp.where(far_ok & here, far_row, -1)
    other_row = jnp.where(far_ok & jnp.logical_not(here), far_row, -1)
    held = mine_ref.shape[0]
    taken = None
    for row, table in ((mine_row, mine_ref), (other_row, other_ref)):
        column = jnp.concatenate([row[:, o : o + 1] for o in range(operators)], axis=0)
        ids = lax.broadcasted_iota(jnp.int32, (operators * slots, held), 1)
        pick = jnp.where(column == ids, 1.0, 0.0).astype(BF16)
        part = jnp.dot(pick, table[...], preferred_element_type=F32)
        taken = part if taken is None else taken + part
    points = trans_ref.shape[1]
    local = None
    for o in range(operators):
        lines = taken[o * slots : (o + 1) * slots]
        both = jnp.concatenate([lines[:, s * points : (s + 1) * points] for s in range(species)], axis=0)
        term = jnp.dot(both.astype(BF16), trans_ref[o], preferred_element_type=F32)
        local = term if local is None else local + term
    total = jnp.dot(local.astype(BF16), down_ref[...], preferred_element_type=F32)

    offset = jnp.where(live & (source >= 0), source - (segment * leaves - MARGIN), -1)
    columns = lax.broadcasted_iota(jnp.int32, (slots, span), 1)
    weights = []
    for o in range(near_mat_ref.shape[0]):
        chosen = jnp.where(kind == o, offset, -1)
        weight = jnp.zeros((slots, span), F32)
        for q in range(source.shape[1]):
            weight = weight + jnp.where(chosen[:, q : q + 1] == columns, 1.0, 0.0)
        weights.append(weight)
    own = []
    around = []
    for s in range(species):
        wide_ref[s, 0:MARGIN, :] = before_ref[s].astype(F32)
        wide_ref[s, MARGIN : MARGIN + leaves, :] = ghosts_ref[s].astype(F32)
        wide_ref[s, MARGIN + leaves : span, :] = after_ref[s].astype(F32)
        own.append(wide_ref[s, MOVE : MOVE + slots, :])
        around.append(wide_ref[s].astype(BF16))
    total = total + jnp.concatenate(own, axis=0)
    rows = species * slots
    for o in range(near_mat_ref.shape[0]):
        weight = weights[o].astype(BF16)
        grouped = jnp.concatenate(
            [jnp.dot(weight, around[s], preferred_element_type=F32) for s in range(species)], axis=0
        )
        rest = grouped - grouped.astype(BF16).astype(F32)
        stacked = jnp.concatenate([grouped, rest], axis=0).astype(BF16)
        term = jnp.dot(stacked, near_mat_ref[o], preferred_element_type=F32)
        total = total + term[:rows] + term[rows:]

    for s in range(species):
        out_ref[s] = jnp.where(live, total[s * slots : (s + 1) * slots], 0.0)


def spaces(text):
    names = {"s": pltpu.SMEM, "v": pltpu.VMEM, "h": pltpu.HBM}
    return [pl.BlockSpec(memory_space=names[c]) for c in text]


def within(mebibytes):
    return pltpu.CompilerParams(vmem_limit_bytes=mebibytes * 1024 * 1024)


def shards(
    coeffs, points, owner_leaf, reaction, fit_matrix, new_seg, near_src, near_op, near_mat, up_mat,
    far_src, trans_mat, down_mat,
):
    species, leaves, width = coeffs.shape
    segments = lax.axis_size(SEG)
    segment = lax.axis_index(SEG)
    part = lax.axis_index("sp")
    parts = lax.axis_size("sp")
    part_id = jnp.full((1,), part, jnp.int32)
    segment_id = jnp.full((1,), segment, jnp.int32)
    slots = segments * CAP
    shape = jax.ShapeDtypeStruct

    request, place = pl.pallas_call(
        route_kernel,
        out_shape=(shape((slots, PB), F32), shape((leaves * BLOCKS,), jnp.int32)),
        in_specs=spaces("shh"),
        out_specs=tuple(spaces("vs")),
        scratch_shapes=[
            pltpu.SMEM((segments,), jnp.int32),
            pltpu.SMEM((BLOCKS, leaves), jnp.int32),
            pltpu.VMEM((leaves, BLOCKS * PB), F32),
            pltpu.VMEM((leaves * BLOCKS, PB), F32),
            pltpu.SemaphoreType.DMA,
            pltpu.SemaphoreType.DMA,
        ],
        compiler_params=within(60),
    )(part_id, owner_leaf.T, points)
    request = lax.all_to_all(request.reshape(segments, CAP, PB), SEG, 0, 0, tiled=True)
    left = pl.pallas_call(
        arrange_kernel,
        out_shape=shape((leaves, 64, 2 * PB), BF16),
        in_specs=spaces("vv"),
        out_specs=spaces("v")[0],
        scratch_shapes=[pltpu.VMEM((leaves * 72, PB), F32)],
        compiler_params=within(8),
    )(coeffs, jnp.asarray(coefficient_table()))
    request = jnp.broadcast_to(request.reshape(1, slots, PB), (parts, slots, PB))
    request = lax.all_to_all(request, "sp", 0, 0, tiled=True)
    index = jnp.clip(request[3, :, 0].astype(jnp.int32), 0, leaves - 1)
    answers = pl.pallas_call(
        functools.partial(evaluate_kernel, species),
        out_shape=shape((slots * species, PB), F32),
        in_specs=spaces("svv"),
        out_specs=spaces("v")[0],
        scratch_shapes=[
            pltpu.VMEM((DEG * 8, PB), F32),
            pltpu.VMEM((8 * 24, PB), F32),
            pltpu.VMEM((8 * 24, PB), F32),
        ],
        compiler_params=within(16),
    )(index, request, left)
    answers = lax.all_to_all(answers.reshape(segments, CAP * species, PB), SEG, 0, 0, tiled=True)
    values = pl.pallas_call(
        collect_kernel,
        out_shape=shape((parts, species, leaves, BLOCKS * PB), F32),
        in_specs=spaces("sv"),
        out_specs=spaces("v")[0],
        scratch_shapes=[pltpu.VMEM((species * leaves * BLOCKS, PB), F32)],
        compiler_params=within(4),
    )(place, answers.reshape(slots * species, PB))
    gathered = lax.all_to_all(values, "sp", 0, 0, tiled=True).reshape(parts * species, leaves, BLOCKS * PB)
    z_size = lax.axis_size("seg_1")
    edge = shape((species, MARGIN, width), BF16)
    slot_total = leaves + 2 * MOVE
    near = near_src.shape[1]
    listed = 2 * near + far_src.shape[1] + 8
    ghosts, first, last, spread, lists = pl.pallas_call(
        fit_kernel,
        out_shape=(
            shape((species, leaves, width), BF16), edge, edge, shape((z_size, leaves, LANES), BF16),
            shape((slot_total, listed), jnp.int32),
        ),
        in_specs=spaces("sssvvvhhhh"),
        out_specs=tuple(spaces("vvvvv")),
        scratch_shapes=[
            pltpu.VMEM((listed - 8, 256), jnp.int32), pltpu.VMEM((1, 256), jnp.int32), pltpu.SemaphoreType.DMA((4,)),
        ],
        compiler_params=within(24),
    )(
        part_id, segment_id, reaction, gathered, fit_matrix, up_mat, near_src.T, near_op.T, far_src.T,
        new_seg.reshape(1, -1),
    )

    up = [(i, i + 1) for i in range(segments - 1)]
    down = [(j, i) for i, j in up]
    before = lax.ppermute(last, SEG, up)
    after = lax.ppermute(first, SEG, down)
    along_z = lax.all_to_all(spread, "seg_1", 0, 0, tiled=True)
    mine = lax.all_gather(along_z.reshape(z_size * leaves, LANES), "seg_0", axis=0, tiled=True)
    other = lax.ppermute(mine, "seg_2", [(0, 1), (1, 0)])

    return pl.pallas_call(
        functools.partial(update_kernel, new_seg.shape[0], near),
        out_shape=shape((species, slot_total, width), F32),
        in_specs=spaces("ssvvvvvvvvv"),
        out_specs=spaces("v")[0],
        scratch_shapes=[pltpu.VMEM((species, leaves + 2 * MARGIN, width), F32)],
        compiler_params=within(10),
    )(
        segment_id, jnp.full((1,), lax.axis_index("seg_2"), jnp.int32), before, ghosts, after, lists, near_mat, mine,
        other, trans_mat, down_mat,
    )


def solution(mesh):
    torus = Mesh(
        mesh.devices.reshape(4, 16, 2, mesh.shape["sp"]), ("seg_0", "seg_1", "seg_2", "sp")
    )
    whole = P()
    return jax.shard_map(
        shards,
        mesh=torus,
        in_specs=(P("sp", SEG, None), P(None, SEG, None), P(SEG, None)) + (whole,) * 10,
        out_specs=P("sp", SEG, None),
        check_vma=False,
    )
```

```python
import functools

import jax
import jax.numpy as jnp
import numpy as np
from jax import lax
from jax.experimental import pallas as pl
from jax.experimental.pallas import tpu as pltpu
from jax.sharding import Mesh
from jax.sharding import PartitionSpec as P


ORDER = 14
DEG = ORDER + 1
BLOCKS = 6
PB = 128
MOVE = 4
REACH = 4
MARGIN = MOVE + REACH
CAP = 2
PAIR_ROWS = 128
LANES = 384
SEG = ("seg_0", "seg_1", "seg_2")
F32 = jnp.float32
BF16 = jnp.bfloat16


def degree_pairs():
    pairs = []
    for i in range(8):
        for r in range(16):
            pairs.append((i, r) if r < DEG - i else (DEG - i, r - (DEG - i)))
    return pairs


def coefficient_table():
    number = {}
    for i in range(DEG):
        for j in range(DEG - i):
            for k in range(DEG - i - j):
                number[i, j, k] = len(number)
    table = np.full((DEG, PAIR_ROWS), -1, np.int32)
    for k in range(DEG):
        for q, (i, j) in enumerate(degree_pairs()):
            if i + j + k <= ORDER:
                table[k, q] = number[i, j, k]
    return table.reshape(1, DEG * PAIR_ROWS)


def high_low(value):
    high = value.astype(BF16)
    return high, (value - high.astype(F32)).astype(BF16)


def polynomials(x):
    terms = [jnp.ones_like(x), x]
    for _ in range(2, DEG):
        terms.append(2.0 * x * terms[-1] - terms[-2])
    return terms


def route_kernel(
    part_ref, owner_hbm, points_ref, request_ref, place_ref, count_ref, owner_ref, plane_ref, line_ref, sem, owner_sem
):
    part = part_ref[0]
    owners = pltpu.make_async_copy(owner_hbm, owner_ref, owner_sem)
    owners.start()
    blocks, leaves = owner_ref.shape
    fetch = pltpu.make_async_copy(points_ref.at[jnp.minimum(part, 2)], plane_ref, sem)
    fetch.start()
    request_ref[...] = jnp.zeros_like(request_ref)

    @pl.loop(0, count_ref.shape[0] // 8)
    def _(d):
        for i in range(8):
            count_ref[d * 8 + i] = 0

    owners.wait()

    @pl.loop(0, leaves)
    def _(leaf):
        for m in range(blocks):
            target = lax.shift_right_logical(owner_ref[m, leaf], 4)
            used = count_ref[target]
            count_ref[target] = used + 1
            place_ref[leaf * blocks + m] = target * CAP + used

    fetch.wait()
    for m in range(blocks):
        line_ref[m * leaves : (m + 1) * leaves] = plane_ref[:, m * PB : (m + 1) * PB]

    @pl.loop(0, leaves)
    def _(leaf):
        for m in range(blocks):
            line = line_ref[pl.ds(m * leaves + leaf, 1), :]
            index = jnp.full((1, PB), (owner_ref[m, leaf] & 15).astype(F32), F32)
            request_ref[pl.ds(place_ref[leaf * blocks + m], 1), :] = jnp.where(part == 3, index, line)


def arrange_kernel(coeffs_ref, table_ref, left_ref, split_ref):
    species, leaves, width = coeffs_ref.shape
    per_leaf = 4 * 16
    stride = per_leaf + 8
    split_ref[...] = jnp.zeros_like(split_ref)
    both = jnp.concatenate([coeffs_ref[s] for s in range(species)], axis=0)
    rest = both - both.astype(BF16).astype(F32)
    stacked = jnp.concatenate([both, rest], axis=0).astype(BF16)
    for k in range(DEG):
        wanted = table_ref[:, k * PAIR_ROWS : (k + 1) * PAIR_ROWS]
        rows = lax.broadcasted_iota(jnp.int32, (width, PAIR_ROWS), 0)
        pick = jnp.where(rows == wanted, 1.0, 0.0).astype(BF16)
        moved = jnp.dot(stacked, pick, preferred_element_type=F32)
        for h in range(2 * species):
            split_ref[pl.ds(h * 16 + k, leaves, stride=stride), :] = moved[h * leaves : (h + 1) * leaves]

    @pl.loop(0, leaves)
    def _(leaf):
        block = split_ref[pl.ds(pl.multiple_of(leaf * stride, 8), per_leaf), :]
        half = per_leaf // 2
        upper = jnp.concatenate([block[:half], jnp.zeros_like(block[:half])], axis=0)
        left_ref[leaf] = jnp.concatenate([block, upper], axis=1).astype(BF16)


def evaluate_kernel(species, index_ref, request_ref, left_ref, out_ref, x_ref, y_ref, z_ref):
    y_ref[...] = jnp.zeros_like(y_ref)
    z_ref[...] = jnp.zeros_like(z_ref)
    row = lax.broadcasted_iota(jnp.int32, (8, PB), 0)

    @pl.loop(0, request_ref.shape[1] // 8)
    def _(group):
        at = pl.ds(pl.multiple_of(group * 8, 8), 8)
        along_x = polynomials(request_ref[0, at, :])
        along_y = polynomials(request_ref[1, at, :])
        along_z = polynomials(request_ref[2, at, :])
        for k in range(DEG):
            x_ref[k * 8 : (k + 1) * 8] = along_x[k]
            y_ref[pl.ds(k, 8, stride=24), :] = along_y[k]
            z_ref[pl.ds(k, 8, stride=24), :] = along_z[k]
        for i in range(8):
            x_rows = [jnp.broadcast_to(x_ref[pl.ds(k * 8 + i, 1), :], (8, PB)) for k in range(DEG)]
            y_first = y_ref[i * 24 : i * 24 + 8]
            y_last = y_ref[i * 24 + 8 : i * 24 + 16]
            products = []
            for b in range(8):
                before = row < DEG - 8 - b
                turned = pltpu.roll(y_first, 7 - b, 0) if b < 7 else y_first
                x_late = x_rows[DEG - b] if b > 0 else x_rows[0]
                products.append(x_rows[b] * y_first)
                products.append(jnp.where(before, x_rows[b], x_late) * jnp.where(before, y_last, turned))
            high, low = high_low(jnp.concatenate(products, axis=0))
            right = jnp.concatenate([high, low], axis=0)
            leaf = index_ref[group * 8 + i]
            sums = jnp.dot(left_ref[leaf], right, preferred_element_type=F32)
            sums = sums[:32] + sums[32:]
            weight = z_ref[i * 24 : i * 24 + 16]
            for s in range(species):
                line = jnp.sum(sums[s * 16 : (s + 1) * 16] * weight, axis=0, keepdims=True)
                out_ref[pl.ds(group * 16 + i * 2 + s, 1), :] = line


def collect_kernel(place_ref, rows_ref, own_ref, out_ref, line_ref):
    copies, species, leaves, _ = out_ref.shape

    @pl.loop(0, leaves)
    def _(leaf):
        for m in range(BLOCKS):
            row = place_ref[leaf * BLOCKS + m]
            for s in range(species):
                at = (s * BLOCKS + m) * leaves + leaf
                line_ref[pl.ds(at, 1), :] = rows_ref[pl.ds(row * species + s, 1), :]

    for s in range(species):
        for m in range(BLOCKS):
            at = (s * BLOCKS + m) * leaves
            piece = line_ref[at : at + leaves]
            own_ref[s, :, m * PB : (m + 1) * PB] = piece
            for c in range(copies):
                out_ref[c, s, :, m * PB : (m + 1) * PB] = piece.astype(BF16)


def parts_kernel(turned_ref, parts_ref):
    parts_ref[0], parts_ref[1] = high_low(turned_ref[...].T)


def fit_kernel(
    part_ref, segment_ref, reaction_ref, own_ref, values_ref, fit_ref, up_ref, near_src_ref, near_op_ref, far_src_ref,
    new_seg_ref, ghosts_ref, first_ref, last_ref, equivalent_ref, lists_ref, window_ref, owned_ref, sems,
):
    part = part_ref[0]
    start = segment_ref[0] * ghosts_ref.shape[1] - MOVE
    window = jnp.clip(lax.shift_right_arithmetic(start, 7) * 128, 0, new_seg_ref.shape[1] - 256)
    window = pl.multiple_of(window, 128)
    fetches = []
    at = 0
    for n, ref in enumerate((near_src_ref, near_op_ref, far_src_ref, new_seg_ref)):
        held = window_ref.at[pl.ds(at, ref.shape[0])] if n < 3 else owned_ref
        fetches.append(pltpu.make_async_copy(ref.at[:, pl.ds(window, 256)], held, sems.at[n]))
        fetches[-1].start()
        at += ref.shape[0]
    all_species = values_ref.shape[0]
    species, leaves, _ = ghosts_ref.shape
    reacted = []
    for s in range(species):
        row = part * species + s
        mixing = reaction_ref[row, 0] * values_ref[0].astype(F32)
        for r in range(1, all_species):
            mixing = mixing + reaction_ref[row, r] * values_ref[r].astype(F32)
        for r in range(species):
            mine = part * species + r
            mixing = mixing + reaction_ref[row, mine] * (own_ref[r] - values_ref[mine].astype(F32))
        reacted.append(own_ref[s] + jnp.tanh(mixing))
    reacted = jnp.concatenate(reacted, axis=0)
    rows = species * leaves
    high = reacted.astype(BF16)
    stacked = jnp.concatenate([reacted, reacted - high.astype(F32)], axis=0).astype(BF16)
    first = jnp.dot(stacked, fit_ref[0], preferred_element_type=F32)
    second = jnp.dot(high, fit_ref[1], preferred_element_type=F32)
    ghosts = (first[:rows] + first[rows:] + second).astype(BF16)
    equivalent = jnp.dot(ghosts, up_ref[...], preferred_element_type=F32).astype(BF16)
    points = up_ref.shape[1]
    for s in range(species):
        here = ghosts[s * leaves : (s + 1) * leaves]
        ghosts_ref[s] = here
        first_ref[s] = here[:MARGIN]
        last_ref[s] = here[leaves - MARGIN :]
    copies, _, lanes = equivalent_ref.shape
    pieces = [equivalent[s * leaves : (s + 1) * leaves] for s in range(species)]
    pieces.append(jnp.zeros((leaves, lanes - species * points), BF16))
    line = jnp.concatenate(pieces, axis=1)
    for c in range(copies):
        equivalent_ref[c] = line
    for fetch in fetches:
        fetch.wait()
    lists = jnp.concatenate([window_ref[...], jnp.broadcast_to(owned_ref[...], (8, 256))], axis=0)
    lists = pltpu.roll(lists, (window - start) & 255, 1)
    lists_ref[...] = lists[:, :128].T[: lists_ref.shape[0]]


def update_kernel(
    total_leaves, near, segment_ref, core_ref, before_ref, ghosts_ref, after_ref, lists_ref, near_mat_ref, mine_ref,
    other_ref, trans_ref, down_ref, out_ref, wide_ref,
):
    segment = segment_ref[0]
    core = core_ref[0]
    species, slots, _ = out_ref.shape
    leaves = ghosts_ref.shape[1]
    span = leaves + 2 * MARGIN
    operators = trans_ref.shape[0]
    start = segment * leaves - MOVE
    lists = lists_ref[...]
    source = lists[:, :near]
    kind = lists[:, near : 2 * near]
    far = lists[:, 2 * near : 2 * near + operators]
    target = start + lax.broadcasted_iota(jnp.int32, (slots, 1), 0)
    live = (target >= 0) & (target < total_leaves) & (lists[:, 2 * near + operators : 2 * near + operators + 1] == segment)

    far_segment = lax.shift_right_logical(far, 4)
    far_row = lax.shift_right_logical(far_segment, 1) * leaves + (far & 15)
    far_ok = live & (far >= 0)
    here = (far_segment & 1) == core
    mine_row = jnp.where(far_ok & here, far_row, -1)
    other_row = jnp.where(far_ok & jnp.logical_not(here), far_row, -1)
    held = mine_ref.shape[0]
    taken = None
    for row, table in ((mine_row, mine_ref), (other_row, other_ref)):
        column = jnp.concatenate([row[:, o : o + 1] for o in range(operators)], axis=0)
        ids = lax.broadcasted_iota(jnp.int32, (operators * slots, held), 1)
        pick = jnp.where(column == ids, 1.0, 0.0).astype(BF16)
        part = jnp.dot(pick, table[...], preferred_element_type=F32)
        taken = part if taken is None else taken + part
    points = trans_ref.shape[1]
    local = None
    for o in range(operators):
        lines = taken[o * slots : (o + 1) * slots]
        both = jnp.concatenate([lines[:, s * points : (s + 1) * points] for s in range(species)], axis=0)
        term = jnp.dot(both.astype(BF16), trans_ref[o], preferred_element_type=F32)
        local = term if local is None else local + term
    total = jnp.dot(local.astype(BF16), down_ref[...], preferred_element_type=F32)

    offset = jnp.where(live & (source >= 0), source - (segment * leaves - MARGIN), -1)
    columns = lax.broadcasted_iota(jnp.int32, (slots, span), 1)
    weights = []
    for o in range(near_mat_ref.shape[0]):
        chosen = jnp.where(kind == o, offset, -1)
        weight = jnp.zeros((slots, span), F32)
        for q in range(source.shape[1]):
            weight = weight + jnp.where(chosen[:, q : q + 1] == columns, 1.0, 0.0)
        weights.append(weight)
    own = []
    around = []
    for s in range(species):
        wide_ref[s, 0:MARGIN, :] = before_ref[s].astype(F32)
        wide_ref[s, MARGIN : MARGIN + leaves, :] = ghosts_ref[s].astype(F32)
        wide_ref[s, MARGIN + leaves : span, :] = after_ref[s].astype(F32)
        own.append(wide_ref[s, MOVE : MOVE + slots, :])
        around.append(wide_ref[s].astype(BF16))
    total = total + jnp.concatenate(own, axis=0)
    rows = species * slots
    for o in range(near_mat_ref.shape[0]):
        weight = weights[o].astype(BF16)
        grouped = jnp.concatenate(
            [jnp.dot(weight, around[s], preferred_element_type=F32) for s in range(species)], axis=0
        )
        rest = grouped - grouped.astype(BF16).astype(F32)
        stacked = jnp.concatenate([grouped, rest], axis=0).astype(BF16)
        term = jnp.dot(stacked, near_mat_ref[o], preferred_element_type=F32)
        total = total + term[:rows] + term[rows:]

    for s in range(species):
        out_ref[s] = jnp.where(live, total[s * slots : (s + 1) * slots], 0.0)


def spaces(text):
    names = {"s": pltpu.SMEM, "v": pltpu.VMEM, "h": pltpu.HBM}
    return [pl.BlockSpec(memory_space=names[c]) for c in text]


def within(mebibytes):
    return pltpu.CompilerParams(vmem_limit_bytes=mebibytes * 1024 * 1024)


def shards(
    coeffs, points, owner_leaf, reaction, fit_matrix, new_seg, near_src, near_op, near_mat, up_mat,
    far_src, trans_mat, down_mat,
):
    species, leaves, width = coeffs.shape
    segments = lax.axis_size(SEG)
    segment = lax.axis_index(SEG)
    part = lax.axis_index("sp")
    parts = lax.axis_size("sp")
    part_id = jnp.full((1,), part, jnp.int32)
    segment_id = jnp.full((1,), segment, jnp.int32)
    slots = segments * CAP
    shape = jax.ShapeDtypeStruct

    request, place = pl.pallas_call(
        route_kernel,
        out_shape=(shape((slots, PB), F32), shape((leaves * BLOCKS,), jnp.int32)),
        in_specs=spaces("shh"),
        out_specs=tuple(spaces("vs")),
        scratch_shapes=[
            pltpu.SMEM((segments,), jnp.int32),
            pltpu.SMEM((BLOCKS, leaves), jnp.int32),
            pltpu.VMEM((leaves, BLOCKS * PB), F32),
            pltpu.VMEM((leaves * BLOCKS, PB), F32),
            pltpu.SemaphoreType.DMA,
            pltpu.SemaphoreType.DMA,
        ],
        compiler_params=within(60),
    )(part_id, owner_leaf.T, points)
    request = lax.all_to_all(request.reshape(segments, CAP, PB), SEG, 0, 0, tiled=True)
    left = pl.pallas_call(
        arrange_kernel,
        out_shape=shape((leaves, 64, 2 * PB), BF16),
        in_specs=spaces("vv"),
        out_specs=spaces("v")[0],
        scratch_shapes=[pltpu.VMEM((leaves * 72, PB), F32)],
        compiler_params=within(8),
    )(coeffs, jnp.asarray(coefficient_table()))
    request = jnp.broadcast_to(request.reshape(1, slots, PB), (parts, slots, PB))
    request = lax.all_to_all(request, "sp", 0, 0, tiled=True)
    index = jnp.clip(request[3, :, 0].astype(jnp.int32), 0, leaves - 1)
    answers = pl.pallas_call(
        functools.partial(evaluate_kernel, species),
        out_shape=shape((slots * species, PB), F32),
        in_specs=spaces("svv"),
        out_specs=spaces("v")[0],
        scratch_shapes=[
            pltpu.VMEM((DEG * 8, PB), F32),
            pltpu.VMEM((8 * 24, PB), F32),
            pltpu.VMEM((8 * 24, PB), F32),
        ],
        compiler_params=within(16),
    )(index, request, left)
    answers = lax.all_to_all(answers.reshape(segments, CAP * species, PB), SEG, 0, 0, tiled=True)
    fit_parts = pl.pallas_call(
        parts_kernel,
        out_shape=shape((2,) + fit_matrix.shape, BF16),
        in_specs=spaces("v"),
        out_specs=spaces("v")[0],
        compiler_params=within(12),
    )(fit_matrix.T)
    own, values = pl.pallas_call(
        collect_kernel,
        out_shape=(
            shape((species, leaves, BLOCKS * PB), F32), shape((parts, species, leaves, BLOCKS * PB), BF16),
        ),
        in_specs=spaces("sv"),
        out_specs=tuple(spaces("vv")),
        scratch_shapes=[pltpu.VMEM((species * leaves * BLOCKS, PB), F32)],
        compiler_params=within(4),
    )(place, answers.reshape(slots * species, PB))
    gathered = lax.all_to_all(values, "sp", 0, 0, tiled=True).reshape(parts * species, leaves, BLOCKS * PB)
    z_size = lax.axis_size("seg_1")
    edge = shape((species, MARGIN, width), BF16)
    slot_total = leaves + 2 * MOVE
    near = near_src.shape[1]
    listed = 2 * near + far_src.shape[1] + 8
    ghosts, first, last, spread, lists = pl.pallas_call(
        fit_kernel,
        out_shape=(
            shape((species, leaves, width), BF16), edge, edge, shape((z_size, leaves, LANES), BF16),
            shape((slot_total, listed), jnp.int32),
        ),
        in_specs=spaces("sssvvvvhhhh"),
        out_specs=tuple(spaces("vvvvv")),
        scratch_shapes=[
            pltpu.VMEM((listed - 8, 256), jnp.int32), pltpu.VMEM((1, 256), jnp.int32), pltpu.SemaphoreType.DMA((4,)),
        ],
        compiler_params=within(24),
    )(
        part_id, segment_id, reaction, own, gathered, fit_parts, up_mat, near_src.T, near_op.T, far_src.T,
        new_seg.reshape(1, -1),
    )

    up = [(i, i + 1) for i in range(segments - 1)]
    down = [(j, i) for i, j in up]
    before = lax.ppermute(last, SEG, up)
    after = lax.ppermute(first, SEG, down)
    along_z = lax.all_to_all(spread, "seg_1", 0, 0, tiled=True)
    mine = lax.all_gather(along_z.reshape(z_size * leaves, LANES), "seg_0", axis=0, tiled=True)
    other = lax.ppermute(mine, "seg_2", [(0, 1), (1, 0)])

    return pl.pallas_call(
        functools.partial(update_kernel, new_seg.shape[0], near),
        out_shape=shape((species, slot_total, width), F32),
        in_specs=spaces("ssvvvvvvvvv"),
        out_specs=spaces("v")[0],
        scratch_shapes=[pltpu.VMEM((species, leaves + 2 * MARGIN, width), F32)],
        compiler_params=within(10),
    )(
        segment_id, jnp.full((1,), lax.axis_index("seg_2"), jnp.int32), before, ghosts, after, lists, near_mat, mine,
        other, trans_mat, down_mat,
    )


def solution(mesh):
    torus = Mesh(
        mesh.devices.reshape(4, 16, 2, mesh.shape["sp"]), ("seg_0", "seg_1", "seg_2", "sp")
    )
    whole = P()
    return jax.shard_map(
        shards,
        mesh=torus,
        in_specs=(P("sp", SEG, None), P(None, SEG, None), P(SEG, None)) + (whole,) * 10,
        out_specs=P("sp", SEG, None),
        check_vma=False,
    )
```

```python
import functools

import jax
import jax.numpy as jnp
import numpy as np
from jax import lax
from jax.experimental import pallas as pl
from jax.experimental.pallas import tpu as pltpu
from jax.sharding import Mesh
from jax.sharding import PartitionSpec as P


ORDER = 14
DEG = ORDER + 1
BLOCKS = 6
PB = 128
MOVE = 4
REACH = 4
MARGIN = MOVE + REACH
CAP = 2
PAIR_ROWS = 128
LANES = 384
SEG = ("seg_0", "seg_1", "seg_2")
F32 = jnp.float32
BF16 = jnp.bfloat16


def degree_pairs():
    pairs = []
    for i in range(8):
        for r in range(16):
            pairs.append((i, r) if r < DEG - i else (DEG - i, r - (DEG - i)))
    return pairs


def coefficient_table():
    number = {}
    for i in range(DEG):
        for j in range(DEG - i):
            for k in range(DEG - i - j):
                number[i, j, k] = len(number)
    table = np.full((DEG, PAIR_ROWS), -1, np.int32)
    for k in range(DEG):
        for q, (i, j) in enumerate(degree_pairs()):
            if i + j + k <= ORDER:
                table[k, q] = number[i, j, k]
    return table.reshape(1, DEG * PAIR_ROWS)


def high_low(value):
    high = value.astype(BF16)
    return high, (value - high.astype(F32)).astype(BF16)


def polynomials(x):
    terms = [jnp.ones_like(x), x]
    for _ in range(2, DEG):
        terms.append(2.0 * x * terms[-1] - terms[-2])
    return terms


def route_kernel(
    part_ref, owner_hbm, points_ref, request_ref, place_ref, count_ref, owner_ref, plane_ref, line_ref, sem, owner_sem
):
    part = part_ref[0]
    owners = pltpu.make_async_copy(owner_hbm, owner_ref, owner_sem)
    owners.start()
    blocks, leaves = owner_ref.shape
    fetch = pltpu.make_async_copy(points_ref.at[jnp.minimum(part, 2)], plane_ref, sem)
    fetch.start()
    request_ref[...] = jnp.zeros_like(request_ref)

    @pl.loop(0, count_ref.shape[0] // 8)
    def _(d):
        for i in range(8):
            count_ref[d * 8 + i] = 0

    owners.wait()

    @pl.loop(0, leaves)
    def _(leaf):
        for m in range(blocks):
            target = lax.shift_right_logical(owner_ref[m, leaf], 4)
            used = count_ref[target]
            count_ref[target] = used + 1
            place_ref[leaf * blocks + m] = target * CAP + used

    fetch.wait()
    for m in range(blocks):
        line_ref[m * leaves : (m + 1) * leaves] = plane_ref[:, m * PB : (m + 1) * PB]

    @pl.loop(0, leaves)
    def _(leaf):
        for m in range(blocks):
            line = line_ref[pl.ds(m * leaves + leaf, 1), :]
            index = jnp.full((1, PB), (owner_ref[m, leaf] & 15).astype(F32), F32)
            request_ref[pl.ds(place_ref[leaf * blocks + m], 1), :] = jnp.where(part == 3, index, line)


def arrange_kernel(coeffs_ref, table_ref, left_ref, split_ref):
    species, leaves, width = coeffs_ref.shape
    per_leaf = 4 * 16
    stride = per_leaf + 8
    split_ref[...] = jnp.zeros_like(split_ref)
    both = jnp.concatenate([coeffs_ref[s] for s in range(species)], axis=0)
    rest = both - both.astype(BF16).astype(F32)
    stacked = jnp.concatenate([both, rest], axis=0).astype(BF16)
    for k in range(DEG):
        wanted = table_ref[:, k * PAIR_ROWS : (k + 1) * PAIR_ROWS]
        rows = lax.broadcasted_iota(jnp.int32, (width, PAIR_ROWS), 0)
        pick = jnp.where(rows == wanted, 1.0, 0.0).astype(BF16)
        moved = jnp.dot(stacked, pick, preferred_element_type=F32)
        for h in range(2 * species):
            split_ref[pl.ds(h * 16 + k, leaves, stride=stride), :] = moved[h * leaves : (h + 1) * leaves]

    @pl.loop(0, leaves)
    def _(leaf):
        block = split_ref[pl.ds(pl.multiple_of(leaf * stride, 8), per_leaf), :]
        half = per_leaf // 2
        upper = jnp.concatenate([block[:half], jnp.zeros_like(block[:half])], axis=0)
        left_ref[leaf] = jnp.concatenate([block, upper], axis=1).astype(BF16)


def evaluate_kernel(species, index_ref, request_ref, left_ref, out_ref, x_ref, y_ref, z_ref):
    y_ref[...] = jnp.zeros_like(y_ref)
    z_ref[...] = jnp.zeros_like(z_ref)
    row = lax.broadcasted_iota(jnp.int32, (8, PB), 0)

    @pl.loop(0, request_ref.shape[1] // 8)
    def _(group):
        at = pl.ds(pl.multiple_of(group * 8, 8), 8)
        along_x = polynomials(request_ref[0, at, :])
        along_y = polynomials(request_ref[1, at, :])
        along_z = polynomials(request_ref[2, at, :])
        for k in range(DEG):
            x_ref[k * 8 : (k + 1) * 8] = along_x[k]
            y_ref[pl.ds(k, 8, stride=24), :] = along_y[k]
            z_ref[pl.ds(k, 8, stride=24), :] = along_z[k]
        for i in range(8):
            x_rows = [jnp.broadcast_to(x_ref[pl.ds(k * 8 + i, 1), :], (8, PB)) for k in range(DEG)]
            y_first = y_ref[i * 24 : i * 24 + 8]
            y_last = y_ref[i * 24 + 8 : i * 24 + 16]
            products = []
            for b in range(8):
                before = row < DEG - 8 - b
                turned = pltpu.roll(y_first, 7 - b, 0) if b < 7 else y_first
                x_late = x_rows[DEG - b] if b > 0 else x_rows[0]
                products.append(x_rows[b] * y_first)
                products.append(jnp.where(before, x_rows[b], x_late) * jnp.where(before, y_last, turned))
            high, low = high_low(jnp.concatenate(products, axis=0))
            right = jnp.concatenate([high, low], axis=0)
            leaf = index_ref[group * 8 + i]
            sums = jnp.dot(left_ref[leaf], right, preferred_element_type=F32)
            sums = sums[:32] + sums[32:]
            weight = z_ref[i * 24 : i * 24 + 16]
            for s in range(species):
                line = jnp.sum(sums[s * 16 : (s + 1) * 16] * weight, axis=0, keepdims=True)
                out_ref[pl.ds(group * 16 + i * 2 + s, 1), :] = line


def collect_kernel(place_ref, rows_ref, own_ref, out_ref, line_ref):
    copies, species, leaves, _ = out_ref.shape

    @pl.loop(0, leaves)
    def _(leaf):
        for m in range(BLOCKS):
            row = place_ref[leaf * BLOCKS + m]
            for s in range(species):
                at = (s * BLOCKS + m) * leaves + leaf
                line_ref[pl.ds(at, 1), :] = rows_ref[pl.ds(row * species + s, 1), :]

    for s in range(species):
        for m in range(BLOCKS):
            at = (s * BLOCKS + m) * leaves
            piece = line_ref[at : at + leaves]
            own_ref[s, :, m * PB : (m + 1) * PB] = piece
            for c in range(copies):
                out_ref[c, s, :, m * PB : (m + 1) * PB] = piece.astype(BF16)


def parts_kernel(turned_ref, parts_ref):
    parts_ref[0], parts_ref[1] = high_low(turned_ref[...].T)


def fit_kernel(
    part_ref, segment_ref, reaction_ref, own_ref, values_ref, fit_ref, up_ref, near_src_ref, near_op_ref, far_src_ref,
    new_seg_ref, ghosts_ref, first_ref, last_ref, equivalent_ref, lists_ref, window_ref, owned_ref, sems,
):
    part = part_ref[0]
    start = segment_ref[0] * ghosts_ref.shape[1] - MOVE
    window = jnp.clip(lax.shift_right_arithmetic(start, 7) * 128, 0, new_seg_ref.shape[1] - 256)
    window = pl.multiple_of(window, 128)
    fetches = []
    at = 0
    for n, ref in enumerate((near_src_ref, near_op_ref, far_src_ref, new_seg_ref)):
        held = window_ref.at[pl.ds(at, ref.shape[0])] if n < 3 else owned_ref
        fetches.append(pltpu.make_async_copy(ref.at[:, pl.ds(window, 256)], held, sems.at[n]))
        fetches[-1].start()
        at += ref.shape[0]
    all_species = values_ref.shape[0]
    species, leaves, _ = ghosts_ref.shape
    reacted = []
    for s in range(species):
        row = part * species + s
        mixing = reaction_ref[row, 0] * values_ref[0].astype(F32)
        for r in range(1, all_species):
            mixing = mixing + reaction_ref[row, r] * values_ref[r].astype(F32)
        for r in range(species):
            mine = part * species + r
            mixing = mixing + reaction_ref[row, mine] * (own_ref[r] - values_ref[mine].astype(F32))
        reacted.append(own_ref[s] + jnp.tanh(mixing))
    reacted = jnp.concatenate(reacted, axis=0)
    rows = species * leaves
    high = reacted.astype(BF16)
    stacked = jnp.concatenate([reacted, reacted - high.astype(F32)], axis=0).astype(BF16)
    first = jnp.dot(stacked, fit_ref[0], preferred_element_type=F32)
    second = jnp.dot(high, fit_ref[1], preferred_element_type=F32)
    ghosts = (first[:rows] + first[rows:] + second).astype(BF16)
    turned = (((1,), (1,)), ((), ()))
    equivalent = lax.dot_general(ghosts, up_ref[...], turned, preferred_element_type=F32).astype(BF16)
    points = up_ref.shape[0]
    for s in range(species):
        here = ghosts[s * leaves : (s + 1) * leaves]
        ghosts_ref[s] = here
        first_ref[s] = here[:MARGIN]
        last_ref[s] = here[leaves - MARGIN :]
    copies, _, lanes = equivalent_ref.shape
    pieces = [equivalent[s * leaves : (s + 1) * leaves] for s in range(species)]
    pieces.append(jnp.zeros((leaves, lanes - species * points), BF16))
    line = jnp.concatenate(pieces, axis=1)
    for c in range(copies):
        equivalent_ref[c] = line
    for fetch in fetches:
        fetch.wait()
    lists = jnp.concatenate([window_ref[...], jnp.broadcast_to(owned_ref[...], (8, 256))], axis=0)
    lists = pltpu.roll(lists, (window - start) & 255, 1)
    lists_ref[...] = lists[:, :128].T[: lists_ref.shape[0]]


def update_kernel(
    total_leaves, near, segment_ref, core_ref, before_ref, ghosts_ref, after_ref, lists_ref, near_mat_ref, mine_ref,
    other_ref, trans_ref, down_ref, out_ref, wide_ref,
):
    segment = segment_ref[0]
    core = core_ref[0]
    species, slots, _ = out_ref.shape
    leaves = ghosts_ref.shape[1]
    span = leaves + 2 * MARGIN
    operators = trans_ref.shape[0]
    start = segment * leaves - MOVE
    lists = lists_ref[...]
    source = lists[:, :near]
    kind = lists[:, near : 2 * near]
    far = lists[:, 2 * near : 2 * near + operators]
    target = start + lax.broadcasted_iota(jnp.int32, (slots, 1), 0)
    live = (target >= 0) & (target < total_leaves) & (lists[:, 2 * near + operators : 2 * near + operators + 1] == segment)

    far_segment = lax.shift_right_logical(far, 4)
    far_row = lax.shift_right_logical(far_segment, 1) * leaves + (far & 15)
    far_ok = live & (far >= 0)
    here = (far_segment & 1) == core
    mine_row = jnp.where(far_ok & here, far_row, -1)
    other_row = jnp.where(far_ok & jnp.logical_not(here), far_row, -1)
    held = mine_ref.shape[0]
    taken = None
    for row, table in ((mine_row, mine_ref), (other_row, other_ref)):
        column = jnp.concatenate([row[:, o : o + 1] for o in range(operators)], axis=0)
        ids = lax.broadcasted_iota(jnp.int32, (operators * slots, held), 1)
        pick = jnp.where(column == ids, 1.0, 0.0).astype(BF16)
        part = jnp.dot(pick, table[...], preferred_element_type=F32)
        taken = part if taken is None else taken + part
    points = trans_ref.shape[1]
    local = None
    for o in range(operators):
        lines = taken[o * slots : (o + 1) * slots]
        both = jnp.concatenate([lines[:, s * points : (s + 1) * points] for s in range(species)], axis=0)
        term = jnp.dot(both.astype(BF16), trans_ref[o], preferred_element_type=F32)
        local = term if local is None else local + term
    total = jnp.dot(local.astype(BF16), down_ref[...], preferred_element_type=F32)

    offset = jnp.where(live & (source >= 0), source - (segment * leaves - MARGIN), -1)
    columns = lax.broadcasted_iota(jnp.int32, (slots, span), 1)
    weights = []
    for o in range(near_mat_ref.shape[0]):
        chosen = jnp.where(kind == o, offset, -1)
        weight = jnp.zeros((slots, span), F32)
        for q in range(source.shape[1]):
            weight = weight + jnp.where(chosen[:, q : q + 1] == columns, 1.0, 0.0)
        weights.append(weight)
    own = []
    around = []
    for s in range(species):
        wide_ref[s, 0:MARGIN, :] = before_ref[s].astype(F32)
        wide_ref[s, MARGIN : MARGIN + leaves, :] = ghosts_ref[s].astype(F32)
        wide_ref[s, MARGIN + leaves : span, :] = after_ref[s].astype(F32)
        own.append(wide_ref[s, MOVE : MOVE + slots, :])
        around.append(wide_ref[s].astype(BF16))
    total = total + jnp.concatenate(own, axis=0)
    rows = species * slots
    for o in range(near_mat_ref.shape[0]):
        weight = weights[o].astype(BF16)
        grouped = jnp.concatenate(
            [jnp.dot(weight, around[s], preferred_element_type=F32) for s in range(species)], axis=0
        )
        rest = grouped - grouped.astype(BF16).astype(F32)
        stacked = jnp.concatenate([grouped, rest], axis=0).astype(BF16)
        term = jnp.dot(stacked, near_mat_ref[o], preferred_element_type=F32)
        total = total + term[:rows] + term[rows:]

    for s in range(species):
        out_ref[s] = jnp.where(live, total[s * slots : (s + 1) * slots], 0.0)


def spaces(text):
    names = {"s": pltpu.SMEM, "v": pltpu.VMEM, "h": pltpu.HBM}
    return [pl.BlockSpec(memory_space=names[c]) for c in text]


def within(mebibytes):
    return pltpu.CompilerParams(vmem_limit_bytes=mebibytes * 1024 * 1024)


def shards(
    coeffs, points, owner_leaf, reaction, fit_matrix, new_seg, near_src, near_op, near_mat, up_mat,
    far_src, trans_mat, down_mat,
):
    species, leaves, width = coeffs.shape
    segments = lax.axis_size(SEG)
    segment = lax.axis_index(SEG)
    part = lax.axis_index("sp")
    parts = lax.axis_size("sp")
    part_id = jnp.full((1,), part, jnp.int32)
    segment_id = jnp.full((1,), segment, jnp.int32)
    slots = segments * CAP
    shape = jax.ShapeDtypeStruct

    request, place = pl.pallas_call(
        route_kernel,
        out_shape=(shape((slots, PB), F32), shape((leaves * BLOCKS,), jnp.int32)),
        in_specs=spaces("shh"),
        out_specs=tuple(spaces("vs")),
        scratch_shapes=[
            pltpu.SMEM((segments,), jnp.int32),
            pltpu.SMEM((BLOCKS, leaves), jnp.int32),
            pltpu.VMEM((leaves, BLOCKS * PB), F32),
            pltpu.VMEM((leaves * BLOCKS, PB), F32),
            pltpu.SemaphoreType.DMA,
            pltpu.SemaphoreType.DMA,
        ],
        compiler_params=within(60),
    )(part_id, owner_leaf.T, points)
    request = lax.all_to_all(request.reshape(segments, CAP, PB), SEG, 0, 0, tiled=True)
    left = pl.pallas_call(
        arrange_kernel,
        out_shape=shape((leaves, 64, 2 * PB), BF16),
        in_specs=spaces("vv"),
        out_specs=spaces("v")[0],
        scratch_shapes=[pltpu.VMEM((leaves * 72, PB), F32)],
        compiler_params=within(8),
    )(coeffs, jnp.asarray(coefficient_table()))
    request = jnp.broadcast_to(request.reshape(1, slots, PB), (parts, slots, PB))
    request = lax.all_to_all(request, "sp", 0, 0, tiled=True)
    index = jnp.clip(request[3, :, 0].astype(jnp.int32), 0, leaves - 1)
    answers = pl.pallas_call(
        functools.partial(evaluate_kernel, species),
        out_shape=shape((slots * species, PB), F32),
        in_specs=spaces("svv"),
        out_specs=spaces("v")[0],
        scratch_shapes=[
            pltpu.VMEM((DEG * 8, PB), F32),
            pltpu.VMEM((8 * 24, PB), F32),
            pltpu.VMEM((8 * 24, PB), F32),
        ],
        compiler_params=within(16),
    )(index, request, left)
    answers = lax.all_to_all(answers.reshape(segments, CAP * species, PB), SEG, 0, 0, tiled=True)
    fit_parts = pl.pallas_call(
        parts_kernel,
        out_shape=shape((2,) + fit_matrix.shape, BF16),
        in_specs=spaces("v"),
        out_specs=spaces("v")[0],
        compiler_params=within(12),
    )(fit_matrix.T)
    own, values = pl.pallas_call(
        collect_kernel,
        out_shape=(
            shape((species, leaves, BLOCKS * PB), F32), shape((parts, species, leaves, BLOCKS * PB), BF16),
        ),
        in_specs=spaces("sv"),
        out_specs=tuple(spaces("vv")),
        scratch_shapes=[pltpu.VMEM((species * leaves * BLOCKS, PB), F32)],
        compiler_params=within(4),
    )(place, answers.reshape(slots * species, PB))
    gathered = lax.all_to_all(values, "sp", 0, 0, tiled=True).reshape(parts * species, leaves, BLOCKS * PB)
    z_size = lax.axis_size("seg_1")
    edge = shape((species, MARGIN, width), BF16)
    slot_total = leaves + 2 * MOVE
    near = near_src.shape[1]
    listed = 2 * near + far_src.shape[1] + 8
    ghosts, first, last, spread, lists = pl.pallas_call(
        fit_kernel,
        out_shape=(
            shape((species, leaves, width), BF16), edge, edge, shape((z_size, leaves, LANES), BF16),
            shape((slot_total, listed), jnp.int32),
        ),
        in_specs=spaces("sssvvvvhhhh"),
        out_specs=tuple(spaces("vvvvv")),
        scratch_shapes=[
            pltpu.VMEM((listed - 8, 256), jnp.int32), pltpu.VMEM((1, 256), jnp.int32), pltpu.SemaphoreType.DMA((4,)),
        ],
        compiler_params=within(24),
    )(
        part_id, segment_id, reaction, own, gathered, fit_parts, up_mat.T, near_src.T, near_op.T, far_src.T,
        new_seg.reshape(1, -1),
    )

    up = [(i, i + 1) for i in range(segments - 1)]
    down = [(j, i) for i, j in up]
    before = lax.ppermute(last, SEG, up)
    after = lax.ppermute(first, SEG, down)
    along_z = lax.all_to_all(spread, "seg_1", 0, 0, tiled=True)
    mine = lax.all_gather(along_z.reshape(z_size * leaves, LANES), "seg_0", axis=0, tiled=True)
    other = lax.ppermute(mine, "seg_2", [(0, 1), (1, 0)])

    return pl.pallas_call(
        functools.partial(update_kernel, new_seg.shape[0], near),
        out_shape=shape((species, slot_total, width), F32),
        in_specs=spaces("ssvvvvvvvvv"),
        out_specs=spaces("v")[0],
        scratch_shapes=[pltpu.VMEM((species, leaves + 2 * MARGIN, width), F32)],
        compiler_params=within(10),
    )(
        segment_id, jnp.full((1,), lax.axis_index("seg_2"), jnp.int32), before, ghosts, after, lists, near_mat, mine,
        other, trans_mat, down_mat,
    )


def solution(mesh):
    torus = Mesh(
        mesh.devices.reshape(4, 16, 2, mesh.shape["sp"]), ("seg_0", "seg_1", "seg_2", "sp")
    )
    whole = P()
    return jax.shard_map(
        shards,
        mesh=torus,
        in_specs=(P("sp", SEG, None), P(None, SEG, None), P(SEG, None)) + (whole,) * 10,
        out_specs=P("sp", SEG, None),
        check_vma=False,
    )
```
